8 devices in a mesh: fsdp: 2 (over z, y), model: 4 (over x, core).
Axes of the slice: x: 2, y: 2, z: 1, core: 2. Of those that a mesh axis runs over, the one named last changes fastest.
Arguments:
- x_in: bfloat16 [16, 1024, 2048], P('fsdp', 'model')
- gain_attn: float32 [2, 2048], replicated
- gain_mlp: float32 [2, 2048], replicated
- rope_cos: float32 [1024, 32], replicated
- rope_sin: float32 [1024, 32], replicated
- w_q: bfloat16 [2, 2048, 2048], P(None, 'fsdp', 'model')
- w_k: bfloat16 [2, 2048, 512], P(None, 'fsdp', 'model')
- w_v: bfloat16 [2, 2048, 512], P(None, 'fsdp', 'model')
- w_o: bfloat16 [2, 2048, 2048], P(None, 'model', 'fsdp')
- w_gate: bfloat16 [2, 2048, 8192], P(None, 'fsdp', 'model')
- w_up: bfloat16 [2, 2048, 8192], P(None, 'fsdp', 'model')
- w_down: bfloat16 [2, 8192, 2048], P(None, 'model', 'fsdp')
Outputs:
- output: bfloat16 [16, 1024, 2048], P('fsdp', 'model')
All inputs are finite; a program needn't handle non-finite values.
Results may differ from the reference program's by a relative error of at most 0.02.
Values are sent between devices in bfloat16 or wider.
A program may use at most 1 GiB of HBM per device.

```python
import math
import jax
import jax.numpy as jnp
from jax import lax

D_MODEL = 2048
FFN = 8192
HEADS = 32
KV_HEADS = 8
HEAD_DIM = 64
BATCH = 16
SEQ = 1024
LAYERS = 2
EPS = 1e-5
ROPE_BASE = 500000.0


def rope_tables(rng_key):
    pos_steps = jax.random.randint(rng_key, (SEQ,), 1, 4)
    positions = (jnp.cumsum(pos_steps) - pos_steps[0]).astype(jnp.float32)
    inv_freq = ROPE_BASE ** (-jnp.arange(HEAD_DIM // 2, dtype=jnp.float32) * (2.0 / HEAD_DIM))
    angles = positions[:, None] * inv_freq[None, :]
    return jnp.cos(angles), jnp.sin(angles)


def setup_inputs(seed: int = 0) -> dict:
    key_list = jax.random.split(jax.random.key(seed), 12)
    q_scale = math.sqrt(max(1.0, math.log(SEQ / 16.0)))

    def normal(rng_key, arr_shape, std_scale):
        return (jax.random.normal(rng_key, arr_shape, jnp.float32) * std_scale).astype(jnp.bfloat16)

    rope_cos, rope_sin = rope_tables(key_list[3])
    return {
        'x_in': normal(key_list[0], (BATCH, SEQ, D_MODEL), 1.0),
        'gain_attn': jax.random.uniform(key_list[1], (LAYERS, D_MODEL), jnp.float32, 0.5, 1.5),
        'gain_mlp': jax.random.uniform(key_list[2], (LAYERS, D_MODEL), jnp.float32, 0.5, 1.5),
        'rope_cos': rope_cos,
        'rope_sin': rope_sin,
        'w_q': normal(key_list[4], (LAYERS, D_MODEL, HEADS * HEAD_DIM), q_scale * D_MODEL ** -0.5),
        'w_k': normal(key_list[5], (LAYERS, D_MODEL, KV_HEADS * HEAD_DIM), D_MODEL ** -0.5),
        'w_v': normal(key_list[6], (LAYERS, D_MODEL, KV_HEADS * HEAD_DIM), D_MODEL ** -0.5),
        'w_o': normal(key_list[7], (LAYERS, HEADS * HEAD_DIM, D_MODEL), 2.0 * (HEADS * HEAD_DIM) ** -0.5),
        'w_gate': normal(key_list[8], (LAYERS, D_MODEL, FFN), D_MODEL ** -0.5),
        'w_up': normal(key_list[9], (LAYERS, D_MODEL, FFN), D_MODEL ** -0.5),
        'w_down': normal(key_list[10], (LAYERS, FFN, D_MODEL), FFN ** -0.5),
    }


def rms_norm(seq_rows, gain_vec):
    rows_f = seq_rows.astype(jnp.float32)
    mean_sq = jnp.mean(rows_f * rows_f, axis=-1, keepdims=True)
    return (rows_f * lax.rsqrt(mean_sq + EPS) * gain_vec).astype(jnp.bfloat16)


def rotate(head_vals, cos_b, sin_b):
    half_dim = head_vals.shape[-1] // 2
    heads_f = head_vals.astype(jnp.float32)
    first_half = heads_f[..., :half_dim]
    second_half = heads_f[..., half_dim:]
    return jnp.concatenate([first_half * cos_b - second_half * sin_b, second_half * cos_b + first_half * sin_b], axis=-1).astype(jnp.bfloat16)


def decoder_layer(seq_rows, params, rope_cos, rope_sin):
    gain_attn, gain_mlp, w_q, w_k, w_v, w_o, w_gate, w_up, w_down = params
    group_size = HEADS // KV_HEADS
    normed = rms_norm(seq_rows, gain_attn)
    q_proj = jnp.dot(normed, w_q, preferred_element_type=jnp.float32).astype(jnp.bfloat16).reshape(SEQ, KV_HEADS, group_size, HEAD_DIM)
    k_proj = jnp.dot(normed, w_k, preferred_element_type=jnp.float32).astype(jnp.bfloat16).reshape(SEQ, KV_HEADS, HEAD_DIM)
    v_proj = jnp.dot(normed, w_v, preferred_element_type=jnp.float32).astype(jnp.bfloat16).reshape(SEQ, KV_HEADS, HEAD_DIM)
    q_rot = rotate(q_proj, rope_cos[:, None, None, :], rope_sin[:, None, None, :])
    k_rot = rotate(k_proj, rope_cos[:, None, :], rope_sin[:, None, :])
    scores = jnp.einsum('qkgd,skd->kgqs', q_rot.astype(jnp.float32), k_rot.astype(jnp.float32)) * HEAD_DIM ** -0.5
    positions = jnp.arange(SEQ)
    causal = positions[:, None] >= positions[None, :]
    scores = jnp.where(causal, scores, -jnp.inf)
    attn_probs = jax.nn.softmax(scores, axis=-1).astype(jnp.bfloat16)
    attn_out = jnp.einsum('kgqs,skd->qkgd', attn_probs.astype(jnp.float32), v_proj.astype(jnp.float32)).astype(jnp.bfloat16).reshape(SEQ, HEADS * HEAD_DIM)
    attn_sum = jnp.dot(attn_out, w_o, preferred_element_type=jnp.float32)
    mid_rows = (seq_rows.astype(jnp.float32) + attn_sum).astype(jnp.bfloat16)
    normed_mlp = rms_norm(mid_rows, gain_mlp)
    gate_acc = jnp.dot(normed_mlp, w_gate, preferred_element_type=jnp.float32)
    up_acc = jnp.dot(normed_mlp, w_up, preferred_element_type=jnp.float32)
    hidden = (jax.nn.silu(gate_acc) * up_acc).astype(jnp.bfloat16)
    mlp_sum = jnp.dot(hidden, w_down, preferred_element_type=jnp.float32)
    return (mid_rows.astype(jnp.float32) + mlp_sum).astype(jnp.bfloat16)


def reference(x_in, gain_attn, gain_mlp, rope_cos, rope_sin, w_q, w_k, w_v, w_o, w_gate, w_up, w_down):
    params = (gain_attn, gain_mlp, w_q, w_k, w_v, w_o, w_gate, w_up, w_down)

    def one_sequence(seq_rows):
        def layer_step(carry_rows, layer_params):
            return decoder_layer(carry_rows, layer_params, rope_cos, rope_sin), None
        final_rows, _ = lax.scan(layer_step, seq_rows, params)
        return final_rows

    return lax.map(one_sequence, x_in)
```

```python
import functools
import math

import jax
import jax.numpy as jnp
from jax import lax
from jax.experimental import pallas as pl
from jax.experimental.pallas import tpu as pltpu
from jax.sharding import PartitionSpec as P


EPS = 1e-5
VMEM = 60 * 1024 * 1024
F32 = jnp.float32
BF16 = jnp.bfloat16


def dot(a, b):
    return jnp.dot(a, b, preferred_element_type=F32)


def params():
    return pltpu.CompilerParams(dimension_semantics=("arbitrary",), vmem_limit_bytes=VMEM)


def normalise(x_ref, gain_ref, h_ref, chunk):
    def step(i, carry):
        rows = pl.ds(pl.multiple_of(i * chunk, chunk), chunk)
        x = x_ref[rows, :].astype(F32)
        mean_sq = jnp.mean(x * x, axis=-1, keepdims=True)
        h_ref[rows, :] = (x * lax.rsqrt(mean_sq + EPS) * gain_ref[...]).astype(BF16)
        return carry

    lax.fori_loop(0, x_ref.shape[0] // chunk, step, 0)


def rotate(x, cos, sin):
    lane = lax.broadcasted_iota(jnp.int32, x.shape, 1)
    swapped = jnp.where(lane % 64 < 32, pltpu.roll(x, 96, 1), pltpu.roll(x, 32, 1))
    return x * cos + swapped * sin


def qkv_kernel(x_ref, gain_ref, cos_ref, sin_ref, w_ref, q_ref, k_ref, v_ref, h_ref):
    @pl.when(pl.program_id(0) == 0)
    def _():
        normalise(x_ref, gain_ref, h_ref, 128)

    w = w_ref[...].reshape(w_ref.shape[0] * w_ref.shape[2], w_ref.shape[3])
    q_width, k_width = q_ref.shape[1], k_ref.shape[1]
    positions = 256
    rows_step = 2 * positions

    def step(i, carry):
        rows = pl.ds(pl.multiple_of(i * rows_step, rows_step), rows_step)
        out = dot(h_ref[rows, :], w).astype(BF16)
        table = pl.ds(pl.multiple_of(i * positions, positions), positions)
        cos, sin = cos_ref[table, :], sin_ref[table, :]
        cos, sin = jnp.concatenate([cos, cos], axis=0), jnp.concatenate([sin, sin], axis=0)
        for c in range(0, q_width, 128):
            q_ref[rows, c:c + 128] = rotate(out[:, c:c + 128].astype(F32), cos, sin).astype(BF16)
        for c in range(0, k_width, 128):
            k_ref[rows, c:c + 128] = rotate(out[:, q_width + c:q_width + c + 128].astype(F32), cos, sin).astype(BF16)
        v_ref[rows, :] = out[:, q_width + k_width:]
        return carry

    lax.fori_loop(0, h_ref.shape[0] // rows_step, step, 0)


def project_qkv(x, gain, cos, sin, w):
    tokens, width = x.shape
    q_width, k_width = 512, 128
    blocks = w.shape[1]
    flops = 2 * tokens * width * blocks * w.shape[3]
    return pl.pallas_call(
        qkv_kernel,
        grid=(blocks,),
        in_specs=[
            pl.BlockSpec((tokens, width), lambda m: (0, 0)),
            pl.BlockSpec((1, width), lambda m: (0, 0)),
            pl.BlockSpec(cos.shape, lambda m: (0, 0)),
            pl.BlockSpec(sin.shape, lambda m: (0, 0)),
            pl.BlockSpec((w.shape[0], 1, w.shape[2], w.shape[3]), lambda m: (0, m, 0, 0)),
        ],
        out_specs=[
            pl.BlockSpec((tokens, q_width), lambda m: (0, m)),
            pl.BlockSpec((tokens, k_width), lambda m: (0, m)),
            pl.BlockSpec((tokens, k_width), lambda m: (0, m)),
        ],
        out_shape=[
            jax.ShapeDtypeStruct((tokens, blocks * q_width), BF16),
            jax.ShapeDtypeStruct((tokens, blocks * k_width), BF16),
            jax.ShapeDtypeStruct((tokens, blocks * k_width), BF16),
        ],
        scratch_shapes=[pltpu.VMEM((tokens, width), BF16)],
        compiler_params=params(),
        cost_estimate=pl.CostEstimate(flops=flops, bytes_accessed=4 * tokens * width + 2 * w.size, transcendentals=0),
        name="qkv",
    )(x, gain, cos, sin, w)


def attention_kernel(q_ref, k_ref, v_ref, o_ref, qs, ks, vs, os):
    chunks, _, chunk, q_width = q_ref.shape
    seq = chunks * chunk
    heads, kv_heads = q_width // 64, k_ref.shape[3] // 64
    for j in range(heads):
        qs[j] = q_ref[:, 0, :, 64 * j:64 * j + 64].reshape(seq, 64)
    for g in range(kv_heads):
        ks[g] = k_ref[:, 0, :, 64 * g:64 * g + 64].reshape(seq, 64)
        vs[g] = v_ref[:, 0, :, 64 * g:64 * g + 64].reshape(seq, 64)
    scale = 64 ** -0.5 * math.log2(math.e)
    row = lax.broadcasted_iota(jnp.int32, (chunk, chunk), 0)
    col = lax.broadcasted_iota(jnp.int32, (chunk, chunk), 1)
    causal = row >= col

    def score(q, k):
        return lax.dot_general(q, k, (((1,), (1,)), ((), ())), preferred_element_type=F32)

    def head(j, carry):
        g = j // (heads // kv_heads)
        for b in range(chunks):
            here = slice(b * chunk, (b + 1) * chunk)
            q = qs[j, here, :]
            diag = jnp.where(causal, score(q, ks[g, here, :]), -jnp.inf)
            top = jnp.max(diag, axis=1, keepdims=True)
            if b:
                past = score(q, ks[g, :b * chunk, :])
                top = jnp.maximum(top, jnp.max(past, axis=1, keepdims=True))
            diag = jnp.exp2((diag - top) * scale)
            total = jnp.sum(diag, axis=1, keepdims=True)
            if b:
                past = jnp.exp2((past - top) * scale)
                total = total + jnp.sum(past, axis=1, keepdims=True)
            inverse = 1.0 / total
            out = dot((diag * inverse).astype(BF16), vs[g, here, :])
            if b:
                out = out + dot((past * inverse).astype(BF16), vs[g, :b * chunk, :])
            os[j, here, :] = out.astype(BF16)
        return carry

    lax.fori_loop(0, heads, head, 0)
    for j in range(heads):
        o_ref[:, 0, :, 64 * j:64 * j + 64] = os[j].reshape(chunks, chunk, 64)


def attend(q, k, v, chunks, seqs):
    tokens = q.shape[0]
    chunk = tokens // (chunks * seqs)
    q4, k4, v4 = (a.reshape(chunks, seqs, chunk, a.shape[1]) for a in (q, k, v))
    seq = chunks * chunk
    blocks = k.shape[1] // 128
    q_width = q.shape[1] // blocks
    heads = q.shape[1] // 64
    out = pl.pallas_call(
        attention_kernel,
        grid=(seqs * blocks,),
        in_specs=[
            pl.BlockSpec((chunks, 1, chunk, q_width), lambda i: (0, i // blocks, 0, i % blocks)),
            pl.BlockSpec((chunks, 1, chunk, 128), lambda i: (0, i // blocks, 0, i % blocks)),
            pl.BlockSpec((chunks, 1, chunk, 128), lambda i: (0, i // blocks, 0, i % blocks)),
        ],
        out_specs=pl.BlockSpec((chunks, 1, chunk, q_width), lambda i: (0, i // blocks, 0, i % blocks)),
        out_shape=jax.ShapeDtypeStruct(q4.shape, BF16),
        scratch_shapes=[
            pltpu.VMEM((q_width // 64, seq, 64), BF16),
            pltpu.VMEM((2, seq, 64), BF16),
            pltpu.VMEM((2, seq, 64), BF16),
            pltpu.VMEM((q_width // 64, seq, 64), BF16),
        ],
        compiler_params=params(),
        cost_estimate=pl.CostEstimate(flops=16 * seqs * heads * seq * seq * 64, bytes_accessed=5 * q.size, transcendentals=seqs * heads * seq * seq),
        name="attention",
    )(q4, k4, v4)
    return out.reshape(q.shape)


def add_matmul_kernel(a_ref, w_ref, r_ref, o_ref, *, chunk):
    w = w_ref[0]
    for r in range(0, a_ref.shape[0], chunk):
        acc = dot(a_ref[r:r + chunk, :], w)
        o_ref[r:r + chunk, :] = (r_ref[r:r + chunk, :].astype(F32) + acc).astype(BF16)


def add_matmul(a, w, resid, part, block, rows):
    tokens, depth = a.shape
    halves, _, cols = w.shape
    per = cols // block
    full = resid.shape[1] // halves // block

    def resid_cols(i):
        y, j = (i // per) % halves, i % per
        return y * full + part * per + j

    steps = halves * per
    return pl.pallas_call(
        functools.partial(add_matmul_kernel, chunk=min(512, rows)),
        grid=(tokens // rows * steps,),
        in_specs=[
            pl.BlockSpec((rows, depth), lambda i: (i // steps, 0)),
            pl.BlockSpec((1, depth, block), lambda i: ((i // per) % halves, 0, i % per)),
            pl.BlockSpec((rows, block), lambda i: (i // steps, resid_cols(i))),
        ],
        out_specs=pl.BlockSpec((rows, block), lambda i: (i // steps, i % steps)),
        out_shape=jax.ShapeDtypeStruct((tokens, halves * cols), BF16),
        compiler_params=params(),
        cost_estimate=pl.CostEstimate(flops=2 * tokens * depth * halves * cols, bytes_accessed=2 * (a.size + w.size), transcendentals=0),
    )(a, w, resid)


def gate_up_kernel(x_ref, gain_ref, wg_ref, wu_ref, z_ref, h_ref, *, chunk):
    @pl.when(pl.program_id(0) == 0)
    def _():
        normalise(x_ref, gain_ref, h_ref, 128)

    depth = wg_ref.shape[0] * wg_ref.shape[2]
    wg = wg_ref[...].reshape(depth, wg_ref.shape[3])
    wu = wu_ref[...].reshape(depth, wu_ref.shape[3])
    for r in range(0, h_ref.shape[0], chunk):
        h = h_ref[r:r + chunk, :]
        gate = dot(h, wg)
        up = dot(h, wu)
        z_ref[r:r + chunk, :] = (gate * jax.nn.sigmoid(gate) * up).astype(BF16)


def gate_up(x, gain, wg, wu):
    tokens, width = x.shape
    ys, blocks, rows, hidden = wg.shape
    block = 512
    per = hidden // block
    w_spec = pl.BlockSpec((ys, 1, rows, block), lambda i: (0, i // per, 0, i % per))
    return pl.pallas_call(
        functools.partial(gate_up_kernel, chunk=512),
        grid=(blocks * per,),
        in_specs=[
            pl.BlockSpec((tokens, width), lambda i: (0, 0)),
            pl.BlockSpec((1, width), lambda i: (0, 0)),
            w_spec,
            w_spec,
        ],
        out_specs=pl.BlockSpec((tokens, block), lambda i: (0, i)),
        out_shape=jax.ShapeDtypeStruct((tokens, blocks * hidden), BF16),
        scratch_shapes=[pltpu.VMEM((tokens, width), BF16)],
        compiler_params=params(),
        cost_estimate=pl.CostEstimate(flops=4 * tokens * width * blocks * hidden, bytes_accessed=2 * (x.size + 2 * wg.size), transcendentals=tokens * blocks * hidden),
    )(x, gain, wg, wu)


def down_kernel(za_ref, zb_ref, w_ref, r_ref, o_ref, *, chunk):
    blocks, _, hidden, cols = w_ref.shape[1:]
    wa = w_ref[0, :, 0].reshape(blocks * hidden, cols)
    wb = w_ref[0, :, 1].reshape(blocks * hidden, cols)
    for r in range(0, za_ref.shape[0], chunk):
        acc = dot(za_ref[r:r + chunk, :], wa) + dot(zb_ref[r:r + chunk, :], wb)
        o_ref[r:r + chunk, :] = (r_ref[r:r + chunk, :].astype(F32) + acc).astype(BF16)


def down(za, zb, w, resid, part, block):
    tokens, depth = za.shape
    ys, blocks, rows_w, cols = w.shape
    w = w.reshape(ys, blocks, 2, rows_w // 2, cols)
    per = cols // block
    full = resid.shape[1] // ys // block
    steps = ys * per
    rows = 1024

    def resid_cols(i):
        return (i // per) % ys * full + part * per + i % per

    return pl.pallas_call(
        functools.partial(down_kernel, chunk=512),
        grid=(tokens // rows * steps,),
        in_specs=[
            pl.BlockSpec((rows, depth), lambda i: (i // steps, 0)),
            pl.BlockSpec((rows, depth), lambda i: (i // steps, 0)),
            pl.BlockSpec((1, blocks, 2, rows_w // 2, block), lambda i: ((i // per) % ys, 0, 0, 0, i % per)),
            pl.BlockSpec((rows, block), lambda i: (i // steps, resid_cols(i))),
        ],
        out_specs=pl.BlockSpec((rows, block), lambda i: (i // steps, i % steps)),
        out_shape=jax.ShapeDtypeStruct((tokens, ys * cols), BF16),
        compiler_params=params(),
        cost_estimate=pl.CostEstimate(flops=4 * tokens * depth * ys * cols, bytes_accessed=2 * (2 * za.size + w.size), transcendentals=0),
    )(za, zb, w, resid)


def solution(mesh):
    act_spec = P('fsdp', 'model', None)
    col_spec = P(None, 'fsdp', 'model')
    row_spec = P(None, 'model', 'fsdp')
    ys, ms = mesh.shape['fsdp'], mesh.shape['model']
    tail_parts = 4

    def gather(block):
        full = lax.all_gather(block, ('fsdp', 'model'), axis=0, tiled=False)
        return full.reshape((ys, ms) + block.shape)

    def exchange(tokens):
        return lax.all_to_all(tokens, 'model', split_axis=0, concat_axis=0, tiled=True)

    def device_step(x_in, gain_attn, gain_mlp, rope_cos, rope_sin, w_q, w_k, w_v, w_o, w_gate, w_up, w_down):
        layers = w_q.shape[0]
        half = w_gate.shape[2] // 2
        seqs = x_in.shape[0] // ms
        x = exchange(x_in)
        gathered = []
        for l in range(layers):
            block = jnp.concatenate([w_q[l], w_k[l], w_v[l]], axis=1)
            wqkv = gather(block)
            wo = gather(w_o[l])
            wgs, wus = [], []
            for h in range(2):
                gate, up = (w[l, :, h * half:(h + 1) * half] for w in (w_gate, w_up))
                wgs.append(gather(gate))
                wus.append(gather(up))
            parts = tail_parts if l == layers - 1 else 1
            cols = w_down.shape[2] // parts
            wds = []
            for c in range(parts):
                block = w_down[l, :, c * cols:(c + 1) * cols]
                wds.append(gather(block))
            gathered.append((wqkv, wo, wgs, wus, wds))

        chunk_shape = x.shape[:2]
        x = x.reshape(-1, x.shape[2])
        cos = jnp.tile(rope_cos, (1, 4))
        sin = jnp.tile(jnp.concatenate([-rope_sin, rope_sin], axis=1), (1, 2))
        for l in range(layers):
            wqkv, wo, wgs, wus, wds = gathered[l]
            q, k, v = project_qkv(x, gain_attn[l][None], cos, sin, wqkv)
            o = attend(q, k, v, ms, seqs)
            m = add_matmul(o, wo.reshape(ys, -1, wo.shape[3]), x, 0, 512, x.shape[0])
            za, zb = (gate_up(m, gain_mlp[l][None], wg, wu) for wg, wu in zip(wgs, wus))
            outs = [down(za, zb, wd, m, c, 256) for c, wd in enumerate(wds)]
            if l < layers - 1:
                x = outs[0]
        cols = outs[0].shape[1] // ys
        outs = [exchange(out.reshape(chunk_shape + (out.shape[1],))) for out in outs]
        return jnp.concatenate([out[:, :, y * cols:(y + 1) * cols] for y in range(ys) for out in outs], axis=2)

    return jax.shard_map(device_step, mesh=mesh, in_specs=(act_spec, P(), P(), P(), P(), col_spec, col_spec, col_spec, row_spec, col_spec, col_spec, row_spec), out_specs=act_spec, check_vma=False)
```

```python
import functools
import math

import jax
import jax.numpy as jnp
from jax import lax
from jax.experimental import pallas as pl
from jax.experimental.pallas import tpu as pltpu
from jax.sharding import PartitionSpec as P


EPS = 1e-5
VMEM = 60 * 1024 * 1024
F32 = jnp.float32
BF16 = jnp.bfloat16


def dot(a, b):
    return jnp.dot(a, b, preferred_element_type=F32)


def params():
    return pltpu.CompilerParams(dimension_semantics=("arbitrary",), vmem_limit_bytes=VMEM)


def normalise(x_ref, gain_ref, h_ref, chunk):
    def step(i, carry):
        rows = pl.ds(pl.multiple_of(i * chunk, chunk), chunk)
        x = x_ref[rows, :].astype(F32)
        mean_sq = jnp.mean(x * x, axis=-1, keepdims=True)
        h_ref[rows, :] = (x * lax.rsqrt(mean_sq + EPS) * gain_ref[...]).astype(BF16)
        return carry

    lax.fori_loop(0, x_ref.shape[0] // chunk, step, 0)


def rotate(x, cos, sin):
    lane = lax.broadcasted_iota(jnp.int32, x.shape, 1)
    swapped = jnp.where(lane % 64 < 32, pltpu.roll(x, 96, 1), pltpu.roll(x, 32, 1))
    return x * cos + swapped * sin


def qkv_kernel(x_ref, gain_ref, cos_ref, sin_ref, w_ref, q_ref, k_ref, v_ref, h_ref):
    @pl.when(pl.program_id(0) == 0)
    def _():
        normalise(x_ref, gain_ref, h_ref, 128)

    w = w_ref[...].reshape(w_ref.shape[0] * w_ref.shape[2], w_ref.shape[3])
    q_width, k_width = q_ref.shape[1], k_ref.shape[1]
    positions = 256
    rows_step = 2 * positions

    def step(i, carry):
        rows = pl.ds(pl.multiple_of(i * rows_step, rows_step), rows_step)
        out = dot(h_ref[rows, :], w).astype(BF16)
        table = pl.ds(pl.multiple_of(i * positions, positions), positions)
        cos, sin = cos_ref[table, :], sin_ref[table, :]
        cos, sin = jnp.concatenate([cos, cos], axis=0), jnp.concatenate([sin, sin], axis=0)
        for c in range(0, q_width, 128):
            q_ref[rows, c:c + 128] = rotate(out[:, c:c + 128].astype(F32), cos, sin).astype(BF16)
        for c in range(0, k_width, 128):
            k_ref[rows, c:c + 128] = rotate(out[:, q_width + c:q_width + c + 128].astype(F32), cos, sin).astype(BF16)
        v_ref[rows, :] = out[:, q_width + k_width:]
        return carry

    lax.fori_loop(0, h_ref.shape[0] // rows_step, step, 0)


def project_qkv(x, gain, cos, sin, w):
    tokens, width = x.shape
    q_width, k_width = 512, 128
    blocks = w.shape[1]
    flops = 2 * tokens * width * blocks * w.shape[3]
    return pl.pallas_call(
        qkv_kernel,
        grid=(blocks,),
        in_specs=[
            pl.BlockSpec((tokens, width), lambda m: (0, 0)),
            pl.BlockSpec((1, width), lambda m: (0, 0)),
            pl.BlockSpec(cos.shape, lambda m: (0, 0)),
            pl.BlockSpec(sin.shape, lambda m: (0, 0)),
            pl.BlockSpec((w.shape[0], 1, w.shape[2], w.shape[3]), lambda m: (0, m, 0, 0)),
        ],
        out_specs=[
            pl.BlockSpec((tokens, q_width), lambda m: (0, m)),
            pl.BlockSpec((tokens, k_width), lambda m: (0, m)),
            pl.BlockSpec((tokens, k_width), lambda m: (0, m)),
        ],
        out_shape=[
            jax.ShapeDtypeStruct((tokens, blocks * q_width), BF16),
            jax.ShapeDtypeStruct((tokens, blocks * k_width), BF16),
            jax.ShapeDtypeStruct((tokens, blocks * k_width), BF16),
        ],
        scratch_shapes=[pltpu.VMEM((tokens, width), BF16)],
        compiler_params=params(),
        cost_estimate=pl.CostEstimate(flops=flops, bytes_accessed=4 * tokens * width + 2 * w.size, transcendentals=0),
        name="qkv",
    )(x, gain, cos, sin, w)


def attention_kernel(q_ref, k_ref, v_ref, o_ref, qs, ks, vs, os):
    chunks, _, chunk, q_width = q_ref.shape
    seq = chunks * chunk
    heads, kv_heads = q_width // 64, k_ref.shape[3] // 64
    for j in range(heads):
        qs[j] = q_ref[:, 0, :, 64 * j:64 * j + 64].reshape(seq, 64)
    for c in range(chunks):
        keys = k_ref[c, 0].astype(F32).T.astype(BF16)
        for g in range(kv_heads):
            ks[g, :, c * chunk:(c + 1) * chunk] = keys[64 * g:64 * g + 64, :]
    for g in range(kv_heads):
        vs[g] = v_ref[:, 0, :, 64 * g:64 * g + 64].reshape(seq, 64)
    scale = 64 ** -0.5 * math.log2(math.e)
    row = lax.broadcasted_iota(jnp.int32, (chunk, chunk), 0)
    col = lax.broadcasted_iota(jnp.int32, (chunk, chunk), 1)
    causal = row >= col

    def head(j, carry):
        g = j // (heads // kv_heads)
        for b in range(chunks):
            q = qs[j, b * chunk:(b + 1) * chunk, :]
            parts = [dot(q, ks[g, :, c * chunk:(c + 1) * chunk]) for c in range(b + 1)]
            parts[b] = jnp.where(causal, parts[b], -jnp.inf)
            top = jnp.max(functools.reduce(jnp.maximum, parts), axis=1, keepdims=True)
            parts = [jnp.exp2((part - top) * scale) for part in parts]
            inverse = 1.0 / jnp.sum(functools.reduce(jnp.add, parts), axis=1, keepdims=True)
            probs = jnp.concatenate([(part * inverse).astype(BF16) for part in parts], axis=1)
            os[j, b * chunk:(b + 1) * chunk, :] = dot(probs, vs[g, :(b + 1) * chunk, :]).astype(BF16)
        return carry

    lax.fori_loop(0, heads, head, 0)
    for j in range(heads):
        o_ref[:, 0, :, 64 * j:64 * j + 64] = os[j].reshape(chunks, chunk, 64)


def attend(q, k, v, chunks, seqs):
    tokens = q.shape[0]
    chunk = tokens // (chunks * seqs)
    q4, k4, v4 = (a.reshape(chunks, seqs, chunk, a.shape[1]) for a in (q, k, v))
    seq = chunks * chunk
    blocks = k.shape[1] // 128
    q_width = q.shape[1] // blocks
    heads = q.shape[1] // 64
    out = pl.pallas_call(
        attention_kernel,
        grid=(seqs * blocks,),
        in_specs=[
            pl.BlockSpec((chunks, 1, chunk, q_width), lambda i: (0, i // blocks, 0, i % blocks)),
            pl.BlockSpec((chunks, 1, chunk, 128), lambda i: (0, i // blocks, 0, i % blocks)),
            pl.BlockSpec((chunks, 1, chunk, 128), lambda i: (0, i // blocks, 0, i % blocks)),
        ],
        out_specs=pl.BlockSpec((chunks, 1, chunk, q_width), lambda i: (0, i // blocks, 0, i % blocks)),
        out_shape=jax.ShapeDtypeStruct(q4.shape, BF16),
        scratch_shapes=[
            pltpu.VMEM((q_width // 64, seq, 64), BF16),
            pltpu.VMEM((2, 64, seq), BF16),
            pltpu.VMEM((2, seq, 64), BF16),
            pltpu.VMEM((q_width // 64, seq, 64), BF16),
        ],
        compiler_params=params(),
        cost_estimate=pl.CostEstimate(flops=16 * seqs * heads * seq * seq * 64, bytes_accessed=5 * q.size, transcendentals=seqs * heads * seq * seq),
        name="attention",
    )(q4, k4, v4)
    return out.reshape(q.shape)


def out_proj_kernel(a_ref, w_ref, r_ref, o_ref, *, chunk):
    w = w_ref[0].reshape(a_ref.shape[1], w_ref.shape[3])
    for r in range(0, a_ref.shape[0], chunk):
        acc = dot(a_ref[r:r + chunk, :], w)
        o_ref[r:r + chunk, :] = (r_ref[r:r + chunk, :].astype(F32) + acc).astype(BF16)


def out_proj(a, w, row_block, resid):
    tokens, depth = a.shape
    ys, ms, _, cols = w.shape
    block = 512
    per = cols // block
    return pl.pallas_call(
        functools.partial(out_proj_kernel, chunk=512),
        grid=(ys * per,),
        in_specs=[
            pl.BlockSpec((tokens, depth), lambda i: (0, 0)),
            pl.BlockSpec((1, ms, depth // ms, block), lambda i: (i // per, 0, row_block, i % per)),
            pl.BlockSpec((tokens, block), lambda i: (0, i)),
        ],
        out_specs=pl.BlockSpec((tokens, block), lambda i: (0, i)),
        out_shape=jax.ShapeDtypeStruct((tokens, ys * cols), BF16),
        compiler_params=params(),
        cost_estimate=pl.CostEstimate(flops=2 * tokens * depth * ys * cols, bytes_accessed=6 * a.size + 2 * depth * ys * cols, transcendentals=0),
        name="out_proj",
    )(a, w, resid)


def gate_up_kernel(x_ref, gain_ref, wg_ref, wu_ref, z_ref, h_ref, *, chunk):
    @pl.when(pl.program_id(0) == 0)
    def _():
        normalise(x_ref, gain_ref, h_ref, 128)

    depth = wg_ref.shape[0] * wg_ref.shape[2]
    wg = wg_ref[...].reshape(depth, wg_ref.shape[3])
    wu = wu_ref[...].reshape(depth, wu_ref.shape[3])
    for r in range(0, h_ref.shape[0], chunk):
        h = h_ref[r:r + chunk, :]
        gate = dot(h, wg)
        up = dot(h, wu)
        z_ref[r:r + chunk, :] = (gate * jax.nn.sigmoid(gate) * up).astype(BF16)


def gate_up(x, gain, w, hidden):
    tokens, width = x.shape
    ys, ms = w.shape[:2]
    rows = width // ys
    block = 512
    per = hidden // block
    return pl.pallas_call(
        functools.partial(gate_up_kernel, chunk=512),
        grid=(ms * per,),
        in_specs=[
            pl.BlockSpec((tokens, width), lambda i: (0, 0)),
            pl.BlockSpec((1, width), lambda i: (0, 0)),
            pl.BlockSpec((ys, 1, rows, block), lambda i: (0, i // per, 0, i % per)),
            pl.BlockSpec((ys, 1, rows, block), lambda i: (0, i // per, 1, i % per)),
        ],
        out_specs=pl.BlockSpec((tokens, block), lambda i: (0, i)),
        out_shape=jax.ShapeDtypeStruct((tokens, ms * hidden), BF16),
        scratch_shapes=[pltpu.VMEM((tokens, width), BF16)],
        compiler_params=params(),
        cost_estimate=pl.CostEstimate(flops=4 * tokens * width * ms * hidden, bytes_accessed=2 * x.size + 4 * width * ms * hidden, transcendentals=tokens * ms * hidden),
    )(x, gain, w, w)


def down_kernel(place_ref, *refs, count, chunk):
    za, zb, ws = refs[:count], refs[count:2 * count], refs[2 * count:3 * count]
    r_ref, o_ref = refs[3 * count], refs[-1]
    half = za[0].shape[1]
    w = jnp.concatenate([w[h * half:(h + 1) * half, :] for h in range(2) for w in ws], axis=0)
    for r in range(0, r_ref.shape[0], chunk):
        z = jnp.concatenate([z[r:r + chunk, :] for z in za + zb], axis=1)
        o_ref[r:r + chunk, :] = (r_ref[r:r + chunk, :].astype(F32) + dot(z, w)).astype(BF16)


def down(place, za, zb, ws, resid, other, onto=None):
    tokens, width = resid.shape
    count = len(ws)
    half = za.shape[1] // count
    cols = ws[0].shape[1]
    block, rows = 256, 1024
    per = cols // block

    def columns(i, place):
        return (i // per, (place[1] ^ other) * per + i % per)

    z_specs = [pl.BlockSpec((rows, half), lambda i, place, k=k: (i // per, place[0] ^ k)) for k in range(count)]
    in_specs = z_specs + z_specs
    in_specs += [pl.BlockSpec((2 * half, block), lambda i, place: (0, i % per))] * count
    in_specs += [pl.BlockSpec((rows, block), columns)]
    operands = [za] * count + [zb] * count + list(ws) + [resid]
    aliases = {}
    if onto is not None:
        in_specs.append(pl.BlockSpec(memory_space=pl.ANY))
        aliases = {1 + len(operands): 0}
        operands.append(onto)
    return pl.pallas_call(
        functools.partial(down_kernel, count=count, chunk=512),
        grid_spec=pltpu.PrefetchScalarGridSpec(
            num_scalar_prefetch=1,
            grid=(tokens // rows * per,),
            in_specs=in_specs,
            out_specs=pl.BlockSpec((rows, block), columns),
        ),
        out_shape=jax.ShapeDtypeStruct((tokens, width), BF16),
        input_output_aliases=aliases,
        compiler_params=params(),
        cost_estimate=pl.CostEstimate(flops=4 * tokens * za.shape[1] * cols, bytes_accessed=4 * za.size + 4 * za.shape[1] * cols, transcendentals=0),
        name="down_other" if other else "down_own",
    )(place, *operands)


def solution(mesh):
    act_spec = P('fsdp', 'model', None)
    col_spec = P(None, 'fsdp', 'model')
    row_spec = P(None, 'model', 'fsdp')
    ys, ms = mesh.shape['fsdp'], mesh.shape['model']

    def gather(block):
        full = lax.all_gather(block, ('fsdp', 'model'), axis=0, tiled=False)
        return full.reshape((ys, ms) + block.shape)

    def exchange(tokens):
        return lax.all_to_all(tokens, 'model', split_axis=0, concat_axis=0, tiled=True)

    def swap(block, axis, bit):
        return lax.ppermute(block, axis, [(i, i ^ bit) for i in range(mesh.shape[axis])])

    def spread(block):
        across = swap(block, 'model', 2)
        over, over_across = swap(block, 'fsdp', 1), swap(across, 'fsdp', 1)
        partners = [swap(b, 'model', 1) for b in (block, across, over, over_across)]
        return (block, partners[0], across, partners[1]), (over, partners[2], over_across, partners[3])

    def device_step(x_in, gain_attn, gain_mlp, rope_cos, rope_sin, w_q, w_k, w_v, w_o, w_gate, w_up, w_down):
        layers = w_q.shape[0]
        half = w_gate.shape[2] // 2
        place = jnp.stack([lax.axis_index('model'), lax.axis_index('fsdp')]).astype(jnp.int32)
        seqs = x_in.shape[0] // ms
        x = exchange(x_in)
        gathered = []
        for l in range(layers):
            block = jnp.concatenate([w_q[l], w_k[l], w_v[l]], axis=1)
            wqkv = gather(block)
            block = jnp.concatenate([w_gate[l, :, :half], w_up[l, :, :half], w_o[l]], axis=0)
            wgua = gather(block)
            block = jnp.concatenate([w_gate[l, :, half:], w_up[l, :, half:]], axis=0)
            wgub = gather(block)
            block = w_down[l]
            gathered.append((wqkv, wgua, wgub, spread(block)))

        chunk_shape = x.shape[:2]
        x = x.reshape(-1, x.shape[2])
        cos = jnp.tile(rope_cos, (1, 4))
        sin = jnp.tile(jnp.concatenate([-rope_sin, rope_sin], axis=1), (1, 2))
        wo_block = 2 * w_gate.shape[1] // w_o.shape[1]
        for l in range(layers):
            wqkv, wgua, wgub, (own, other) = gathered[l]
            q, k, v = project_qkv(x, gain_attn[l][None], cos, sin, wqkv)
            o = attend(q, k, v, ms, seqs)
            m = out_proj(o, wgua, wo_block, x)
            if l == layers - 1:
                m = exchange(m.reshape(chunk_shape + m.shape[1:])).reshape(m.shape)
            za = gate_up(m, gain_mlp[l][None], wgua, half)
            zb = gate_up(m, gain_mlp[l][None], wgub, half)
            x = down(place, za, zb, own, m, 0)
            x = down(place, za, zb, other, m, 1, x)
        return x.reshape(x_in.shape)

    return jax.shard_map(device_step, mesh=mesh, in_specs=(act_spec, P(), P(), P(), P(), col_spec, col_spec, col_spec, row_spec, col_spec, col_spec, row_spec), out_specs=act_spec, check_vma=False)
```

```python
import functools
import math

import jax
import jax.numpy as jnp
from jax import lax
from jax.experimental import pallas as pl
from jax.experimental.pallas import tpu as pltpu
from jax.sharding import PartitionSpec as P


EPS = 1e-5
VMEM = 60 * 1024 * 1024
F32 = jnp.float32
BF16 = jnp.bfloat16


def dot(a, b):
    return jnp.dot(a, b, preferred_element_type=F32)


def params():
    return pltpu.CompilerParams(dimension_semantics=("arbitrary",), vmem_limit_bytes=VMEM)


def normalise(x_ref, gain_ref, h_ref, chunk):
    def step(i, carry):
        rows = pl.ds(pl.multiple_of(i * chunk, chunk), chunk)
        x = x_ref[rows, :].astype(F32)
        mean_sq = jnp.mean(x * x, axis=-1, keepdims=True)
        h_ref[rows, :] = (x * lax.rsqrt(mean_sq + EPS) * gain_ref[...]).astype(BF16)
        return carry

    lax.fori_loop(0, x_ref.shape[0] // chunk, step, 0)


def rotate(x, cos, sin):
    lane = lax.broadcasted_iota(jnp.int32, x.shape, 1)
    swapped = jnp.where(lane % 64 < 32, pltpu.roll(x, 96, 1), pltpu.roll(x, 32, 1))
    return x * cos + swapped * sin


def qkv_kernel(x_ref, gain_ref, cos_ref, sin_ref, w_ref, q_ref, k_ref, v_ref, h_ref):
    @pl.when(pl.program_id(0) == 0)
    def _():
        normalise(x_ref, gain_ref, h_ref, 128)

    w = w_ref[...].reshape(w_ref.shape[0] * w_ref.shape[2], w_ref.shape[3])
    q_width, k_width = q_ref.shape[1], k_ref.shape[1]
    positions = 256
    step = 2 * positions
    for r in range(0, h_ref.shape[0], step):
        rows = slice(r, r + step)
        out = dot(h_ref[rows, :], w).astype(BF16)
        table = slice(r // 2, r // 2 + positions)
        cos, sin = cos_ref[table, :], sin_ref[table, :]
        cos, sin = jnp.concatenate([cos, cos], axis=0), jnp.concatenate([sin, sin], axis=0)
        for c in range(0, q_width, 128):
            q_ref[rows, c:c + 128] = rotate(out[:, c:c + 128].astype(F32), cos, sin).astype(BF16)
        for c in range(0, k_width, 128):
            k_ref[rows, c:c + 128] = rotate(out[:, q_width + c:q_width + c + 128].astype(F32), cos, sin).astype(BF16)
        v_ref[rows, :] = out[:, q_width + k_width:]


def project_qkv(x, gain, cos, sin, w):
    tokens, width = x.shape
    q_width, k_width = 512, 128
    blocks = w.shape[1]
    flops = 2 * tokens * width * blocks * w.shape[3]
    return pl.pallas_call(
        qkv_kernel,
        grid=(blocks,),
        in_specs=[
            pl.BlockSpec((tokens, width), lambda m: (0, 0)),
            pl.BlockSpec((1, width), lambda m: (0, 0)),
            pl.BlockSpec(cos.shape, lambda m: (0, 0)),
            pl.BlockSpec(sin.shape, lambda m: (0, 0)),
            pl.BlockSpec((w.shape[0], 1, w.shape[2], w.shape[3]), lambda m: (0, m, 0, 0)),
        ],
        out_specs=[
            pl.BlockSpec((tokens, q_width), lambda m: (0, m)),
            pl.BlockSpec((tokens, k_width), lambda m: (0, m)),
            pl.BlockSpec((tokens, k_width), lambda m: (0, m)),
        ],
        out_shape=[
            jax.ShapeDtypeStruct((tokens, blocks * q_width), BF16),
            jax.ShapeDtypeStruct((tokens, blocks * k_width), BF16),
            jax.ShapeDtypeStruct((tokens, blocks * k_width), BF16),
        ],
        scratch_shapes=[pltpu.VMEM((tokens, width), BF16)],
        compiler_params=params(),
        cost_estimate=pl.CostEstimate(flops=flops, bytes_accessed=4 * tokens * width + 2 * w.size, transcendentals=0),
        name="qkv",
    )(x, gain, cos, sin, w)


def attention_kernel(q_ref, k_ref, v_ref, o_ref, ks, vs):
    chunks, _, chunk, _ = q_ref.shape
    lo = lax.broadcasted_iota(jnp.int32, (chunk, 128), 1) < 64
    for c in range(chunks):
        rows = slice(c * chunk, (c + 1) * chunk)
        keys = k_ref[c, 0].astype(F32).T.astype(BF16)
        values = v_ref[c, 0].astype(F32)
        swapped = pltpu.roll(values, 64, 1)
        for g in range(2):
            key = keys[64 * g:64 * g + 64, :]
            ks[g, :, rows] = jnp.concatenate([key, key], axis=0)
            first, second = (swapped, values) if g else (values, swapped)
            vs[g, 0, rows, :] = jnp.where(lo, first, 0.0).astype(BF16)
            vs[g, 1, rows, :] = jnp.where(lo, 0.0, second).astype(BF16)
    scale = 64 ** -0.5 * math.log2(math.e)
    row = lax.broadcasted_iota(jnp.int32, (4 * chunk, chunk), 0) % chunk
    col = lax.broadcasted_iota(jnp.int32, (4 * chunk, chunk), 1)
    causal = row >= col

    def group(g, carry):
        for b in range(chunks):
            n = (b + 1) * chunk
            heads = []
            for p in range(2):
                pair = q_ref[b, 0, :, pl.ds(pl.multiple_of(g * 256 + p * 128, 128), 128)].astype(F32)
                heads += [jnp.where(lo, pair, 0.0).astype(BF16), jnp.where(lo, 0.0, pair).astype(BF16)]
            q = jnp.concatenate(heads, axis=0)
            parts = [dot(q, ks[g, :, c * chunk:(c + 1) * chunk]) for c in range(b + 1)]
            parts[b] = jnp.where(causal, parts[b], -jnp.inf)
            top = jnp.max(functools.reduce(jnp.maximum, parts), axis=1, keepdims=True)
            parts = [jnp.exp2((part - top) * scale) for part in parts]
            inverse = 1.0 / jnp.sum(functools.reduce(jnp.add, parts), axis=1, keepdims=True)
            probs = [(part * inverse).astype(BF16) for part in parts]
            values = jnp.concatenate([vs[g, 0, :n, :], vs[g, 1, :n, :]], axis=0)
            for p in range(2):
                even, odd = 2 * p * chunk, (2 * p + 1) * chunk
                pair = jnp.concatenate([x[even:even + chunk] for x in probs] + [x[odd:odd + chunk] for x in probs], axis=1)
                o_ref[b, 0, :, pl.ds(pl.multiple_of(g * 256 + p * 128, 128), 128)] = dot(pair, values).astype(BF16)
        return carry

    lax.fori_loop(0, 2, group, 0)


def attend(q, k, v, chunks, seqs, only):
    tokens = q.shape[0]
    chunk = tokens // (chunks * seqs)
    q4, k4, v4 = (a.reshape(chunks, seqs, chunk, a.shape[1]) for a in (q, k, v))
    seq = chunks * chunk
    blocks = k.shape[1] // 128
    q_width = q.shape[1] // blocks
    heads = q.shape[1] // 64
    count = seqs if only is None else 1
    first = only or 0
    out = pl.pallas_call(
        attention_kernel,
        grid=(count * blocks,),
        in_specs=[
            pl.BlockSpec((chunks, 1, chunk, width), lambda i: (0, first + i // blocks, 0, i % blocks))
            for width in (q_width, 128, 128)
        ],
        out_specs=pl.BlockSpec((chunks, 1, chunk, q_width), lambda i: (0, i // blocks, 0, i % blocks)),
        out_shape=jax.ShapeDtypeStruct((chunks, count, chunk, q.shape[1]), BF16),
        scratch_shapes=[
            pltpu.VMEM((2, 128, seq), BF16),
            pltpu.VMEM((2, 2, seq, 128), BF16),
        ],
        compiler_params=params(),
        cost_estimate=pl.CostEstimate(flops=8 * count * heads * seq * seq * 64, bytes_accessed=5 * count * seq * q.shape[1], transcendentals=count * heads * seq * seq),
    )(q4, k4, v4)
    return out.reshape(count * seq, q.shape[1])


def out_proj_kernel(a_ref, w_ref, r_ref, o_ref, *, chunk):
    w = w_ref[0].reshape(a_ref.shape[1], w_ref.shape[3])
    resid = r_ref[...].reshape(o_ref.shape)
    for r in range(0, a_ref.shape[0], chunk):
        acc = dot(a_ref[r:r + chunk, :], w)
        o_ref[r:r + chunk, :] = (resid[r:r + chunk, :].astype(F32) + acc).astype(BF16)


def out_proj(a, w, row_block, resid, only):
    tokens, depth = a.shape
    ys, ms, _, cols = w.shape
    block = 512
    per = cols // block
    chunks, seqs, chunk, _ = resid.shape
    count = seqs if only is None else 1
    first = only or 0
    return pl.pallas_call(
        functools.partial(out_proj_kernel, chunk=512),
        grid=(ys * per,),
        in_specs=[
            pl.BlockSpec((tokens, depth), lambda i: (0, 0)),
            pl.BlockSpec((1, ms, depth // ms, block), lambda i: (i // per, 0, row_block, i % per)),
            pl.BlockSpec((chunks, count, chunk, block), lambda i: (0, first, 0, i)),
        ],
        out_specs=pl.BlockSpec((tokens, block), lambda i: (0, i)),
        out_shape=jax.ShapeDtypeStruct((tokens, ys * cols), BF16),
        compiler_params=params(),
        cost_estimate=pl.CostEstimate(flops=2 * tokens * depth * ys * cols, bytes_accessed=6 * a.size + 2 * depth * ys * cols, transcendentals=0),
    )(a, w, resid)


def gate_up_kernel(x_ref, gain_ref, wg_ref, wu_ref, *refs, chunk):
    z_ref, h_ref = refs[-2:]

    @pl.when(pl.program_id(0) == 0)
    def _():
        normalise(x_ref, gain_ref, h_ref, 128)

    depth = wg_ref.shape[0] * wg_ref.shape[2]
    wg = wg_ref[...].reshape(depth, wg_ref.shape[3])
    wu = wu_ref[...].reshape(depth, wu_ref.shape[3])
    for r in range(0, h_ref.shape[0], chunk):
        h = h_ref[r:r + chunk, :]
        gate = dot(h, wg)
        up = dot(h, wu)
        z_ref[r:r + chunk, :] = (gate * jax.nn.sigmoid(gate) * up).astype(BF16)


def gate_up(x, gain, w, hidden, parts=1, part=0, onto=None):
    tokens, width = x.shape
    ys, ms = w.shape[:2]
    rows = width // ys
    block = 512
    per = hidden // block
    in_specs = [
        pl.BlockSpec((tokens, width), lambda i: (0, 0)),
        pl.BlockSpec((1, width), lambda i: (0, 0)),
        pl.BlockSpec((ys, 1, rows, block), lambda i: (0, i // per, 0, i % per)),
        pl.BlockSpec((ys, 1, rows, block), lambda i: (0, i // per, 1, i % per)),
    ]
    operands = [x, gain, w, w]
    aliases = {}
    if onto is not None:
        in_specs.append(pl.BlockSpec(memory_space=pl.ANY))
        operands.append(onto)
        aliases = {4: 0}
    return pl.pallas_call(
        functools.partial(gate_up_kernel, chunk=512),
        grid=(ms * per,),
        in_specs=in_specs,
        out_specs=pl.BlockSpec((tokens, block), lambda i: (part, i)),
        out_shape=jax.ShapeDtypeStruct((parts * tokens, ms * hidden), BF16),
        scratch_shapes=[pltpu.VMEM((tokens, width), BF16)],
        input_output_aliases=aliases,
        compiler_params=params(),
        cost_estimate=pl.CostEstimate(flops=4 * tokens * width * ms * hidden, bytes_accessed=2 * x.size + 4 * width * ms * hidden, transcendentals=tokens * ms * hidden),
    )(*operands)


def down_kernel(place_ref, *refs, count, resids, steps, chunk):
    za, zb, ws = refs[:count], refs[count:2 * count], refs[2 * count:3 * count]
    r_refs, o_ref = refs[3 * count:3 * count + resids], refs[-1]
    half = za[0].shape[1]
    w = jnp.concatenate([w[h * half:(h + 1) * half, :] for h in range(2) for w in ws], axis=0)
    for r in range(0, za[0].shape[0], chunk):
        rows = slice(r, r + chunk)
        z = jnp.concatenate([z[rows, :] for z in za + zb], axis=1)
        resid = r_refs[0][rows, :].astype(F32)
        if resids == 2:
            resid = jnp.where(pl.program_id(0) < steps, resid, r_refs[1][rows, :].astype(F32))
        out = (resid + dot(z, w)).astype(BF16)
        if len(o_ref.shape) == 4:
            positions = o_ref.shape[2]
            o_ref[r // positions:(r + chunk) // positions, 0] = out.reshape(chunk // positions, positions, out.shape[1])
        else:
            o_ref[rows, :] = out


def down(place, za, zb, ws, resids, other, split, onto=None):
    tokens = za.shape[0]
    width = resids[0].shape[1]
    count = len(ws)
    half = za.shape[1] // count
    cols = ws[0].shape[1]
    block, rows = 256, 1024
    per = cols // block

    def column(i, place):
        return (place[1] ^ other) * per + i % per

    z_specs = [pl.BlockSpec((rows, half), lambda i, place, k=k: (i // per, place[0] ^ k)) for k in range(count)]
    in_specs = z_specs + z_specs
    in_specs += [pl.BlockSpec((2 * half, block), lambda i, place: (0, i % per))] * count
    if len(resids) == 1:
        in_specs += [pl.BlockSpec((rows, block), lambda i, place: (i // per, column(i, place)))]
    else:
        in_specs += [pl.BlockSpec((rows, block), lambda i, place: (0, column(i, place)))] * len(resids)
    operands = [za] * count + [zb] * count + list(ws) + list(resids)
    aliases = {}
    if onto is not None:
        in_specs.append(pl.BlockSpec(memory_space=pl.ANY))
        aliases = {1 + len(operands): 0}
        operands.append(onto)
    if split:
        out_spec = pl.BlockSpec((split, 1, rows // split, block), lambda i, place: (0, i // per, 0, column(i, place)))
        out_shape = (split, tokens // rows, rows // split, width)
    else:
        out_spec = pl.BlockSpec((rows, block), lambda i, place: (i // per, column(i, place)))
        out_shape = (tokens, width)
    return pl.pallas_call(
        functools.partial(down_kernel, count=count, resids=len(resids), steps=per, chunk=512),
        grid_spec=pltpu.PrefetchScalarGridSpec(
            num_scalar_prefetch=1,
            grid=(tokens // rows * per,),
            in_specs=in_specs,
            out_specs=out_spec,
        ),
        out_shape=jax.ShapeDtypeStruct(out_shape, BF16),
        input_output_aliases=aliases,
        compiler_params=params(),
        cost_estimate=pl.CostEstimate(flops=4 * tokens * za.shape[1] * cols, bytes_accessed=4 * za.size + 4 * za.shape[1] * cols, transcendentals=0),
        name="down_other" if other else "down_own",
    )(place, *operands)


def solution(mesh):
    act_spec = P('fsdp', 'model', None)
    col_spec = P(None, 'fsdp', 'model')
    row_spec = P(None, 'model', 'fsdp')
    ys, ms = mesh.shape['fsdp'], mesh.shape['model']

    def gather(block):
        full = lax.all_gather(block, ('fsdp', 'model'), axis=0, tiled=False)
        return full.reshape((ys, ms) + block.shape)

    def exchange(tokens):
        return lax.all_to_all(tokens, 'model', split_axis=0, concat_axis=0, tiled=True)

    def swap(block, axis, bit):
        return lax.ppermute(block, axis, [(i, i ^ bit) for i in range(mesh.shape[axis])])

    def spread(block):
        across = swap(block, 'model', 2)
        over, over_across = swap(block, 'fsdp', 1), swap(across, 'fsdp', 1)
        partners = [swap(b, 'model', 1) for b in (block, across, over, over_across)]
        return (block, partners[0], across, partners[1]), (over, partners[2], over_across, partners[3])

    def device_step(x_in, gain_attn, gain_mlp, rope_cos, rope_sin, w_q, w_k, w_v, w_o, w_gate, w_up, w_down):
        layers = w_q.shape[0]
        half = w_gate.shape[2] // 2
        place = jnp.stack([lax.axis_index('model'), lax.axis_index('fsdp')]).astype(jnp.int32)
        seqs = x_in.shape[0] // ms
        x = exchange(x_in)
        gathered = []
        for l in range(layers):
            block = jnp.concatenate([w_q[l], w_k[l], w_v[l]], axis=1)
            wqkv = gather(block)
            block = jnp.concatenate([w_gate[l, :, :half], w_up[l, :, :half], w_o[l]], axis=0)
            wgua = gather(block)
            block = jnp.concatenate([w_gate[l, :, half:], w_up[l, :, half:]], axis=0)
            wgub = gather(block)
            block = w_down[l]
            gathered.append((wqkv, wgua, wgub, spread(block)))

        x = x.reshape(-1, x.shape[2])
        cos = jnp.tile(rope_cos, (1, 4))
        sin = jnp.tile(jnp.concatenate([-rope_sin, rope_sin], axis=1), (1, 2))
        wo_block = 2 * w_gate.shape[1] // w_o.shape[1]
        for l in range(layers):
            wqkv, wgua, wgub, (own, other) = gathered[l]
            gain = gain_mlp[l][None]
            q, k, v = project_qkv(x, gain_attn[l][None], cos, sin, wqkv)
            x4 = x.reshape(ms, seqs, -1, x.shape[1])
            if l < layers - 1:
                o = attend(q, k, v, ms, seqs, None)
                resids = [out_proj(o, wgua, wo_block, x4, None)]
                split = None
            else:
                resids, split = [], ms
                for i in range(seqs):
                    o = attend(q, k, v, ms, seqs, i)
                    m = out_proj(o, wgua, wo_block, x4, i)
                    resids.append(exchange(m.reshape(ms, -1, m.shape[1])).reshape(m.shape))
            za = zb = None
            for i, m in enumerate(resids):
                za = gate_up(m, gain, wgua, half, len(resids), i, za)
            for i, m in enumerate(resids):
                zb = gate_up(m, gain, wgub, half, len(resids), i, zb)
            x = down(place, za, zb, own, resids, 0, split)
            x = down(place, za, zb, other, resids, 1, split, x)
        return x.reshape(x_in.shape)

    return jax.shard_map(device_step, mesh=mesh, in_specs=(act_spec, P(), P(), P(), P(), col_spec, col_spec, col_spec, row_spec, col_spec, col_spec, row_spec), out_specs=act_spec, check_vma=False)
```

```python
import functools
import math

import jax
import jax.numpy as jnp
from jax import lax
from jax.experimental import pallas as pl
from jax.experimental.pallas import tpu as pltpu
from jax.sharding import PartitionSpec as P


EPS = 1e-5
VMEM = 60 * 1024 * 1024
F32 = jnp.float32
BF16 = jnp.bfloat16


def dot(a, b):
    return jnp.dot(a, b, preferred_element_type=F32)


def params():
    return pltpu.CompilerParams(dimension_semantics=("arbitrary",), vmem_limit_bytes=VMEM)


def normalise(x_ref, gain_ref, h_ref, chunk):
    def step(i, carry):
        rows = pl.ds(pl.multiple_of(i * chunk, chunk), chunk)
        x = x_ref[rows, :].astype(F32)
        mean_sq = jnp.mean(x * x, axis=-1, keepdims=True)
        h_ref[rows, :] = (x * lax.rsqrt(mean_sq + EPS) * gain_ref[...]).astype(BF16)
        return carry

    lax.fori_loop(0, x_ref.shape[0] // chunk, step, 0)


def rotate(x, cos, sin):
    lane = lax.broadcasted_iota(jnp.int32, x.shape, 1)
    swapped = jnp.where(lane % 64 < 32, pltpu.roll(x, 96, 1), pltpu.roll(x, 32, 1))
    return x * cos + swapped * sin


def qkv_kernel(x_ref, gain_ref, cos_ref, sin_ref, w_ref, q_ref, k_ref, v_ref, h_ref):
    @pl.when(pl.program_id(0) == 0)
    def _():
        normalise(x_ref, gain_ref, h_ref, 128)

    w = w_ref[...].reshape(w_ref.shape[0] * w_ref.shape[2], w_ref.shape[3])
    q_width, k_width = q_ref.shape[1], k_ref.shape[1]
    positions = 256
    step = 2 * positions
    for r in range(0, h_ref.shape[0], step):
        rows = slice(r, r + step)
        out = dot(h_ref[rows, :], w).astype(BF16)
        table = slice(r // 2, r // 2 + positions)
        cos, sin = cos_ref[table, :], sin_ref[table, :]
        cos, sin = jnp.concatenate([cos, cos], axis=0), jnp.concatenate([sin, sin], axis=0)
        for c in range(0, q_width, 128):
            q_ref[rows, c:c + 128] = rotate(out[:, c:c + 128].astype(F32), cos, sin).astype(BF16)
        for c in range(0, k_width, 128):
            k_ref[rows, c:c + 128] = rotate(out[:, q_width + c:q_width + c + 128].astype(F32), cos, sin).astype(BF16)
        v_ref[rows, :] = out[:, q_width + k_width:]


def project_qkv(x, gain, cos, sin, w):
    tokens, width = x.shape
    q_width, k_width = 512, 128
    blocks = w.shape[1]
    flops = 2 * tokens * width * blocks * w.shape[3]
    return pl.pallas_call(
        qkv_kernel,
        grid=(blocks,),
        in_specs=[
            pl.BlockSpec((tokens, width), lambda m: (0, 0)),
            pl.BlockSpec((1, width), lambda m: (0, 0)),
            pl.BlockSpec(cos.shape, lambda m: (0, 0)),
            pl.BlockSpec(sin.shape, lambda m: (0, 0)),
            pl.BlockSpec((w.shape[0], 1, w.shape[2], w.shape[3]), lambda m: (0, m, 0, 0)),
        ],
        out_specs=[
            pl.BlockSpec((tokens, q_width), lambda m: (0, m)),
            pl.BlockSpec((tokens, k_width), lambda m: (0, m)),
            pl.BlockSpec((tokens, k_width), lambda m: (0, m)),
        ],
        out_shape=[
            jax.ShapeDtypeStruct((tokens, blocks * q_width), BF16),
            jax.ShapeDtypeStruct((tokens, blocks * k_width), BF16),
            jax.ShapeDtypeStruct((tokens, blocks * k_width), BF16),
        ],
        scratch_shapes=[pltpu.VMEM((tokens, width), BF16)],
        compiler_params=params(),
        cost_estimate=pl.CostEstimate(flops=flops, bytes_accessed=4 * tokens * width + 2 * w.size, transcendentals=0),
        name="qkv",
    )(x, gain, cos, sin, w)


def attention_kernel(q_ref, k_ref, v_ref, o_ref, ks, vs):
    chunks, _, chunk, _ = q_ref.shape
    lo = lax.broadcasted_iota(jnp.int32, (chunk, 128), 1) < 64
    for c in range(chunks):
        rows = slice(c * chunk, (c + 1) * chunk)
        keys = k_ref[c, 0].astype(F32).T.astype(BF16)
        values = v_ref[c, 0].astype(F32)
        swapped = pltpu.roll(values, 64, 1)
        for g in range(2):
            key = keys[64 * g:64 * g + 64, :]
            ks[g, :, rows] = jnp.concatenate([key, key], axis=0)
            first, second = (swapped, values) if g else (values, swapped)
            vs[g, 0, rows, :] = jnp.where(lo, first, 0.0).astype(BF16)
            vs[g, 1, rows, :] = jnp.where(lo, 0.0, second).astype(BF16)
    scale = 64 ** -0.5 * math.log2(math.e)
    row = lax.broadcasted_iota(jnp.int32, (4 * chunk, chunk), 0) % chunk
    col = lax.broadcasted_iota(jnp.int32, (4 * chunk, chunk), 1)
    causal = row >= col

    def group(g, carry):
        for b in range(chunks):
            n = (b + 1) * chunk
            heads = []
            for p in range(2):
                pair = q_ref[b, 0, :, pl.ds(pl.multiple_of(g * 256 + p * 128, 128), 128)].astype(F32)
                heads += [jnp.where(lo, pair, 0.0).astype(BF16), jnp.where(lo, 0.0, pair).astype(BF16)]
            q = jnp.concatenate(heads, axis=0)
            parts = [dot(q, ks[g, :, c * chunk:(c + 1) * chunk]) for c in range(b + 1)]
            parts[b] = jnp.where(causal, parts[b], -jnp.inf)
            top = jnp.max(functools.reduce(jnp.maximum, parts), axis=1, keepdims=True)
            parts = [jnp.exp2((part - top) * scale) for part in parts]
            inverse = 1.0 / jnp.sum(functools.reduce(jnp.add, parts), axis=1, keepdims=True)
            probs = [(part * inverse).astype(BF16) for part in parts]
            values = jnp.concatenate([vs[g, 0, :n, :], vs[g, 1, :n, :]], axis=0)
            for p in range(2):
                even, odd = 2 * p * chunk, (2 * p + 1) * chunk
                pair = jnp.concatenate([x[even:even + chunk] for x in probs] + [x[odd:odd + chunk] for x in probs], axis=1)
                o_ref[b, 0, :, pl.ds(pl.multiple_of(g * 256 + p * 128, 128), 128)] = dot(pair, values).astype(BF16)
        return carry

    lax.fori_loop(0, 2, group, 0)


def attend(q, k, v, chunks, seqs, only):
    tokens = q.shape[0]
    chunk = tokens // (chunks * seqs)
    q4, k4, v4 = (a.reshape(chunks, seqs, chunk, a.shape[1]) for a in (q, k, v))
    seq = chunks * chunk
    blocks = k.shape[1] // 128
    q_width = q.shape[1] // blocks
    heads = q.shape[1] // 64
    count = seqs if only is None else 1
    first = only or 0
    out = pl.pallas_call(
        attention_kernel,
        grid=(count * blocks,),
        in_specs=[
            pl.BlockSpec((chunks, 1, chunk, width), lambda i: (0, first + i // blocks, 0, i % blocks))
            for width in (q_width, 128, 128)
        ],
        out_specs=pl.BlockSpec((chunks, 1, chunk, q_width), lambda i: (0, i // blocks, 0, i % blocks)),
        out_shape=jax.ShapeDtypeStruct((chunks, count, chunk, q.shape[1]), BF16),
        scratch_shapes=[
            pltpu.VMEM((2, 128, seq), BF16),
            pltpu.VMEM((2, 2, seq, 128), BF16),
        ],
        compiler_params=params(),
        cost_estimate=pl.CostEstimate(flops=8 * count * heads * seq * seq * 64, bytes_accessed=5 * count * seq * q.shape[1], transcendentals=count * heads * seq * seq),
    )(q4, k4, v4)
    return out.reshape(count * seq, q.shape[1])


def out_proj_kernel(a_ref, w_ref, r_ref, o_ref, *, chunk):
    w = w_ref[0].reshape(a_ref.shape[1], w_ref.shape[3])
    resid = r_ref[...].reshape(o_ref.shape)
    for r in range(0, a_ref.shape[0], chunk):
        acc = dot(a_ref[r:r + chunk, :], w)
        o_ref[r:r + chunk, :] = (resid[r:r + chunk, :].astype(F32) + acc).astype(BF16)


def out_proj(a, w, row_block, resid, only):
    tokens, depth = a.shape
    ys, ms, _, cols = w.shape
    block = 512
    per = cols // block
    chunks, seqs, chunk, _ = resid.shape
    count = seqs if only is None else 1
    first = only or 0
    return pl.pallas_call(
        functools.partial(out_proj_kernel, chunk=512),
        grid=(ys * per,),
        in_specs=[
            pl.BlockSpec((tokens, depth), lambda i: (0, 0)),
            pl.BlockSpec((1, ms, depth // ms, block), lambda i: (i // per, 0, row_block, i % per)),
            pl.BlockSpec((chunks, count, chunk, block), lambda i: (0, first, 0, i)),
        ],
        out_specs=pl.BlockSpec((tokens, block), lambda i: (0, i)),
        out_shape=jax.ShapeDtypeStruct((tokens, ys * cols), BF16),
        compiler_params=params(),
        cost_estimate=pl.CostEstimate(flops=2 * tokens * depth * ys * cols, bytes_accessed=6 * a.size + 2 * depth * ys * cols, transcendentals=0),
    )(a, w, resid)


def gate_up_kernel(x_ref, gain_ref, wg_ref, wu_ref, *refs, chunk):
    z_ref, h_ref = refs[-2:]

    @pl.when(pl.program_id(0) == 0)
    def _():
        normalise(x_ref, gain_ref, h_ref, 128)

    depth = wg_ref.shape[0] * wg_ref.shape[2]
    wg = wg_ref[...].reshape(depth, wg_ref.shape[3])
    wu = wu_ref[...].reshape(depth, wu_ref.shape[3])
    for r in range(0, h_ref.shape[0], chunk):
        h = h_ref[r:r + chunk, :]
        gate = dot(h, wg)
        up = dot(h, wu)
        z_ref[r:r + chunk, :] = (gate * jax.nn.sigmoid(gate) * up).astype(BF16)


def gate_up(x, gain, w, hidden, parts=1, part=0, onto=None):
    tokens, width = x.shape
    ys, ms = w.shape[:2]
    rows = width // ys
    block = 512
    per = hidden // block
    in_specs = [
        pl.BlockSpec((tokens, width), lambda i: (0, 0)),
        pl.BlockSpec((1, width), lambda i: (0, 0)),
        pl.BlockSpec((ys, 1, rows, block), lambda i: (0, i // per, 0, i % per)),
        pl.BlockSpec((ys, 1, rows, block), lambda i: (0, i // per, 1, i % per)),
    ]
    operands = [x, gain, w, w]
    aliases = {}
    if onto is not None:
        in_specs.append(pl.BlockSpec(memory_space=pl.ANY))
        operands.append(onto)
        aliases = {4: 0}
    return pl.pallas_call(
        functools.partial(gate_up_kernel, chunk=512),
        grid=(ms * per,),
        in_specs=in_specs,
        out_specs=pl.BlockSpec((tokens, block), lambda i: (part, i)),
        out_shape=jax.ShapeDtypeStruct((parts * tokens, ms * hidden), BF16),
        scratch_shapes=[pltpu.VMEM((tokens, width), BF16)],
        input_output_aliases=aliases,
        compiler_params=params(),
        cost_estimate=pl.CostEstimate(flops=4 * tokens * width * ms * hidden, bytes_accessed=2 * x.size + 4 * width * ms * hidden, transcendentals=tokens * ms * hidden),
    )(*operands)


def down_kernel(place_ref, *refs, count, resids, steps, chunk):
    za, zb, ws = refs[:count], refs[count:2 * count], refs[2 * count:3 * count]
    r_refs, o_ref = refs[3 * count:3 * count + resids], refs[-1]
    half = za[0].shape[1]
    w = jnp.concatenate([w[h * half:(h + 1) * half, :] for h in range(2) for w in ws], axis=0)
    for r in range(0, za[0].shape[0], chunk):
        rows = slice(r, r + chunk)
        z = jnp.concatenate([z[rows, :] for z in za + zb], axis=1)
        resid = r_refs[0][rows, :].astype(F32)
        if resids == 2:
            resid = jnp.where(pl.program_id(0) < steps, resid, r_refs[1][rows, :].astype(F32))
        out = (resid + dot(z, w)).astype(BF16)
        if len(o_ref.shape) == 4:
            positions = o_ref.shape[2]
            o_ref[r // positions:(r + chunk) // positions, 0] = out.reshape(chunk // positions, positions, out.shape[1])
        else:
            o_ref[rows, :] = out


def down(place, za, zb, ws, resids, split, other=0, part=0, parts=1, onto=None):
    tokens = za.shape[0]
    width = resids[0].shape[1]
    whole = not isinstance(ws, (list, tuple))
    count = ws.shape[1] if whole else len(ws)
    halves = ws.shape[0] if whole else 1
    cols = ws.shape[3] if whole else ws[0].shape[1]
    half = za.shape[1] // count
    block, rows = 256, 1024
    per = cols // block
    steps = halves * per

    def column(i, place):
        y = i // per % halves if whole else place[1] ^ other
        return (y * parts + part) * per + i % per

    def source(k, place):
        return k if whole else place[0] ^ k

    z_specs = [pl.BlockSpec((rows, half), lambda i, place, k=k: (i // steps, source(k, place))) for k in range(count)]
    in_specs = z_specs + z_specs
    if whole:
        in_specs += [pl.BlockSpec((None, None, 2 * half, block), lambda i, place, k=k: (i // per % halves, k, 0, i % per)) for k in range(count)]
        operands = [za] * count + [zb] * count + [ws] * count + list(resids)
    else:
        in_specs += [pl.BlockSpec((2 * half, block), lambda i, place: (0, i % per))] * count
        operands = [za] * count + [zb] * count + list(ws) + list(resids)
    if len(resids) == 1:
        in_specs += [pl.BlockSpec((rows, block), lambda i, place: (i // steps, column(i, place)))]
    else:
        in_specs += [pl.BlockSpec((rows, block), lambda i, place: (0, column(i, place)))] * len(resids)
    aliases = {}
    if onto is not None:
        in_specs.append(pl.BlockSpec(memory_space=pl.ANY))
        aliases = {1 + len(operands): 0}
        operands.append(onto)
    if split:
        out_spec = pl.BlockSpec((split, 1, rows // split, block), lambda i, place: (0, i // steps, 0, column(i, place)))
        out_shape = (split, tokens // rows, rows // split, width)
    else:
        out_spec = pl.BlockSpec((rows, block), lambda i, place: (i // steps, column(i, place)))
        out_shape = (tokens, width)
    return pl.pallas_call(
        functools.partial(down_kernel, count=count, resids=len(resids), steps=steps, chunk=512),
        grid_spec=pltpu.PrefetchScalarGridSpec(
            num_scalar_prefetch=1,
            grid=(tokens // rows * steps,),
            in_specs=in_specs,
            out_specs=out_spec,
        ),
        out_shape=jax.ShapeDtypeStruct(out_shape, BF16),
        input_output_aliases=aliases,
        compiler_params=params(),
        cost_estimate=pl.CostEstimate(flops=4 * tokens * za.shape[1] * halves * cols, bytes_accessed=4 * za.size + 4 * za.shape[1] * halves * cols, transcendentals=0),
    )(place, *operands)


def solution(mesh):
    act_spec = P('fsdp', 'model', None)
    col_spec = P(None, 'fsdp', 'model')
    row_spec = P(None, 'model', 'fsdp')
    ys, ms = mesh.shape['fsdp'], mesh.shape['model']

    def gather(block):
        full = lax.all_gather(block, ('fsdp', 'model'), axis=0, tiled=False)
        return full.reshape((ys, ms) + block.shape)

    def exchange(tokens):
        return lax.all_to_all(tokens, 'model', split_axis=0, concat_axis=0, tiled=True)

    def swap(block, axis, bit):
        return lax.ppermute(block, axis, [(i, i ^ bit) for i in range(mesh.shape[axis])])

    def spread(block):
        across = swap(block, 'model', 2)
        over, over_across = swap(block, 'fsdp', 1), swap(across, 'fsdp', 1)
        partners = [swap(b, 'model', 1) for b in (block, across, over, over_across)]
        return (block, partners[0], across, partners[1]), (over, partners[2], over_across, partners[3])

    def device_step(x_in, gain_attn, gain_mlp, rope_cos, rope_sin, w_q, w_k, w_v, w_o, w_gate, w_up, w_down):
        layers = w_q.shape[0]
        half = w_gate.shape[2] // 2
        place = jnp.stack([lax.axis_index('model'), lax.axis_index('fsdp')]).astype(jnp.int32)
        seqs = x_in.shape[0] // ms
        x = exchange(x_in)
        gathered = []
        for l in range(layers):
            last = l == layers - 1
            block = jnp.concatenate([w_q[l], w_k[l], w_v[l]], axis=1)
            wqkv = gather(block)
            if last:
                wo = gather(w_o[l])
            block = jnp.concatenate([w_gate[l, :, :half], w_up[l, :, :half]] + ([] if last else [w_o[l]]), axis=0)
            wgua = gather(block)
            if not last:
                wo = wgua
            block = jnp.concatenate([w_gate[l, :, half:], w_up[l, :, half:]], axis=0)
            wgub = gather(block)
            cols = w_down.shape[2] // (2 if last else 1)
            block = w_down[l, :, :cols]
            rest = w_down[l, :, cols:]
            wd = spread(block)
            gathered.append((wqkv, wo, wgua, wgub, wd, gather(rest) if last else None))

        x = x.reshape(-1, x.shape[2])
        cos = jnp.tile(rope_cos, (1, 4))
        sin = jnp.tile(jnp.concatenate([-rope_sin, rope_sin], axis=1), (1, 2))
        for l in range(layers):
            wqkv, wo, wgua, wgub, (own, other), rest = gathered[l]
            gain = gain_mlp[l][None]
            wo_block = wo.shape[2] // w_o.shape[1] - 1
            parts = 1 if rest is None else 2
            q, k, v = project_qkv(x, gain_attn[l][None], cos, sin, wqkv)
            x4 = x.reshape(ms, seqs, -1, x.shape[1])
            if l < layers - 1:
                o = attend(q, k, v, ms, seqs, None)
                resids = [out_proj(o, wo, wo_block, x4, None)]
                split = None
            else:
                resids, split = [], ms
                for i in range(seqs):
                    o = attend(q, k, v, ms, seqs, i)
                    m = out_proj(o, wo, wo_block, x4, i)
                    resids.append(exchange(m.reshape(ms, -1, m.shape[1])).reshape(m.shape))
            za = zb = None
            for i, m in enumerate(resids):
                za = gate_up(m, gain, wgua, half, len(resids), i, za)
            for i, m in enumerate(resids):
                zb = gate_up(m, gain, wgub, half, len(resids), i, zb)
            x = down(place, za, zb, own, resids, split, 0, 0, parts)
            x = down(place, za, zb, other, resids, split, 1, 0, parts, x)
            if rest is not None:
                x = down(place, za, zb, rest, resids, split, 0, 1, parts, x)
        return x.reshape(x_in.shape)

    return jax.shard_map(device_step, mesh=mesh, in_specs=(act_spec, P(), P(), P(), P(), col_spec, col_spec, col_spec, row_spec, col_spec, col_spec, row_spec), out_specs=act_spec, check_vma=False)
```

```python
import functools
import math

import jax
import jax.numpy as jnp
from jax import lax
from jax.experimental import pallas as pl
from jax.experimental.pallas import tpu as pltpu
from jax.sharding import PartitionSpec as P


EPS = 1e-5
VMEM = 60 * 1024 * 1024
F32 = jnp.float32
BF16 = jnp.bfloat16


def dot(a, b):
    return jnp.dot(a, b, preferred_element_type=F32)


def params():
    return pltpu.CompilerParams(dimension_semantics=("arbitrary",), vmem_limit_bytes=VMEM)


def normalise(x_ref, gain_ref, h_ref, chunk):
    def step(i, carry):
        rows = pl.ds(pl.multiple_of(i * chunk, chunk), chunk)
        x = x_ref[rows, :].astype(F32)
        mean_sq = jnp.mean(x * x, axis=-1, keepdims=True)
        h_ref[rows, :] = (x * lax.rsqrt(mean_sq + EPS) * gain_ref[...]).astype(BF16)
        return carry

    lax.fori_loop(0, x_ref.shape[0] // chunk, step, 0)


def rotate(x, cos, sin):
    lane = lax.broadcasted_iota(jnp.int32, x.shape, 1)
    swapped = jnp.where(lane % 64 < 32, pltpu.roll(x, 96, 1), pltpu.roll(x, 32, 1))
    return x * cos + swapped * sin


def qkv_kernel(x_ref, gain_ref, cos_ref, sin_ref, w_ref, q_ref, k_ref, v_ref, h_ref):
    @pl.when(pl.program_id(0) == 0)
    def _():
        normalise(x_ref, gain_ref, h_ref, 128)

    w = w_ref[...].reshape(w_ref.shape[0] * w_ref.shape[2], w_ref.shape[3])
    q_width, k_width = q_ref.shape[1], k_ref.shape[1]
    positions = 256
    step = 2 * positions
    for r in range(0, h_ref.shape[0], step):
        rows = slice(r, r + step)
        out = dot(h_ref[rows, :], w).astype(BF16)
        table = slice(r // 2, r // 2 + positions)
        cos, sin = cos_ref[table, :], sin_ref[table, :]
        cos, sin = jnp.concatenate([cos, cos], axis=0), jnp.concatenate([sin, sin], axis=0)
        for c in range(0, q_width, 128):
            q_ref[rows, c:c + 128] = rotate(out[:, c:c + 128].astype(F32), cos, sin).astype(BF16)
        for c in range(0, k_width, 128):
            k_ref[rows, c:c + 128] = rotate(out[:, q_width + c:q_width + c + 128].astype(F32), cos, sin).astype(BF16)
        v_ref[rows, :] = out[:, q_width + k_width:]


def project_qkv(x, gain, cos, sin, w):
    tokens, width = x.shape
    q_width, k_width = 512, 128
    blocks = w.shape[1]
    flops = 2 * tokens * width * blocks * w.shape[3]
    return pl.pallas_call(
        qkv_kernel,
        grid=(blocks,),
        in_specs=[
            pl.BlockSpec((tokens, width), lambda m: (0, 0)),
            pl.BlockSpec((1, width), lambda m: (0, 0)),
            pl.BlockSpec(cos.shape, lambda m: (0, 0)),
            pl.BlockSpec(sin.shape, lambda m: (0, 0)),
            pl.BlockSpec((w.shape[0], 1, w.shape[2], w.shape[3]), lambda m: (0, m, 0, 0)),
        ],
        out_specs=[
            pl.BlockSpec((tokens, q_width), lambda m: (0, m)),
            pl.BlockSpec((tokens, k_width), lambda m: (0, m)),
            pl.BlockSpec((tokens, k_width), lambda m: (0, m)),
        ],
        out_shape=[
            jax.ShapeDtypeStruct((tokens, blocks * q_width), BF16),
            jax.ShapeDtypeStruct((tokens, blocks * k_width), BF16),
            jax.ShapeDtypeStruct((tokens, blocks * k_width), BF16),
        ],
        scratch_shapes=[pltpu.VMEM((tokens, width), BF16)],
        compiler_params=params(),
        cost_estimate=pl.CostEstimate(flops=flops, bytes_accessed=4 * tokens * width + 2 * w.size, transcendentals=0),
        name="qkv",
    )(x, gain, cos, sin, w)


def attention_kernel(q_ref, k_ref, v_ref, o_ref, ks, vs):
    chunks, _, chunk, _ = q_ref.shape
    lo = lax.broadcasted_iota(jnp.int32, (chunk, 128), 1) < 64
    for c in range(chunks):
        rows = slice(c * chunk, (c + 1) * chunk)
        keys = k_ref[c, 0].astype(F32).T.astype(BF16)
        values = v_ref[c, 0].astype(F32)
        swapped = pltpu.roll(values, 64, 1)
        for g in range(2):
            key = keys[64 * g:64 * g + 64, :]
            ks[g, :, rows] = jnp.concatenate([key, key], axis=0)
            first, second = (swapped, values) if g else (values, swapped)
            vs[g, 0, rows, :] = jnp.where(lo, first, 0.0).astype(BF16)
            vs[g, 1, rows, :] = jnp.where(lo, 0.0, second).astype(BF16)
    scale = 64 ** -0.5 * math.log2(math.e)
    row = lax.broadcasted_iota(jnp.int32, (4 * chunk, chunk), 0) % chunk
    col = lax.broadcasted_iota(jnp.int32, (4 * chunk, chunk), 1)
    causal = row >= col

    def group(g, carry):
        for b in range(chunks):
            n = (b + 1) * chunk
            heads = []
            for p in range(2):
                pair = q_ref[b, 0, :, pl.ds(pl.multiple_of(g * 256 + p * 128, 128), 128)].astype(F32)
                heads += [jnp.where(lo, pair, 0.0).astype(BF16), jnp.where(lo, 0.0, pair).astype(BF16)]
            q = jnp.concatenate(heads, axis=0)
            parts = [dot(q, ks[g, :, c * chunk:(c + 1) * chunk]) for c in range(b + 1)]
            parts[b] = jnp.where(causal, parts[b], -jnp.inf)
            top = jnp.max(functools.reduce(jnp.maximum, parts), axis=1, keepdims=True)
            parts = [jnp.exp2((part - top) * scale) for part in parts]
            inverse = 1.0 / jnp.sum(functools.reduce(jnp.add, parts), axis=1, keepdims=True)
            probs = [(part * inverse).astype(BF16) for part in parts]
            values = jnp.concatenate([vs[g, 0, :n, :], vs[g, 1, :n, :]], axis=0)
            for p in range(2):
                even, odd = 2 * p * chunk, (2 * p + 1) * chunk
                pair = jnp.concatenate([x[even:even + chunk] for x in probs] + [x[odd:odd + chunk] for x in probs], axis=1)
                o_ref[b, 0, :, pl.ds(pl.multiple_of(g * 256 + p * 128, 128), 128)] = dot(pair, values).astype(BF16)
        return carry

    lax.fori_loop(0, 2, group, 0)


def attend(q, k, v, chunks, seqs, only):
    tokens = q.shape[0]
    chunk = tokens // (chunks * seqs)
    q4, k4, v4 = (a.reshape(chunks, seqs, chunk, a.shape[1]) for a in (q, k, v))
    seq = chunks * chunk
    blocks = k.shape[1] // 128
    q_width = q.shape[1] // blocks
    heads = q.shape[1] // 64
    count = seqs if only is None else 1
    first = only or 0
    out = pl.pallas_call(
        attention_kernel,
        grid=(count * blocks,),
        in_specs=[
            pl.BlockSpec((chunks, 1, chunk, width), lambda i: (0, first + i // blocks, 0, i % blocks))
            for width in (q_width, 128, 128)
        ],
        out_specs=pl.BlockSpec((chunks, 1, chunk, q_width), lambda i: (0, i // blocks, 0, i % blocks)),
        out_shape=jax.ShapeDtypeStruct((chunks, count, chunk, q.shape[1]), BF16),
        scratch_shapes=[
            pltpu.VMEM((2, 128, seq), BF16),
            pltpu.VMEM((2, 2, seq, 128), BF16),
        ],
        compiler_params=params(),
        cost_estimate=pl.CostEstimate(flops=8 * count * heads * seq * seq * 64, bytes_accessed=5 * count * seq * q.shape[1], transcendentals=count * heads * seq * seq),
    )(q4, k4, v4)
    return out.reshape(count * seq, q.shape[1])


def out_proj_kernel(a_ref, w_ref, r_ref, o_ref, *, chunk):
    w = w_ref[0].reshape(a_ref.shape[1], w_ref.shape[3])
    resid = r_ref[...].reshape(o_ref.shape)
    for r in range(0, a_ref.shape[0], chunk):
        acc = dot(a_ref[r:r + chunk, :], w)
        o_ref[r:r + chunk, :] = (resid[r:r + chunk, :].astype(F32) + acc).astype(BF16)


def out_proj(a, w, row_block, resid, only):
    tokens, depth = a.shape
    ys, ms, _, cols = w.shape
    block = 512
    per = cols // block
    chunks, seqs, chunk, _ = resid.shape
    count = seqs if only is None else 1
    first = only or 0
    return pl.pallas_call(
        functools.partial(out_proj_kernel, chunk=512),
        grid=(ys * per,),
        in_specs=[
            pl.BlockSpec((tokens, depth), lambda i: (0, 0)),
            pl.BlockSpec((1, ms, depth // ms, block), lambda i: (i // per, 0, row_block, i % per)),
            pl.BlockSpec((chunks, count, chunk, block), lambda i: (0, first, 0, i)),
        ],
        out_specs=pl.BlockSpec((tokens, block), lambda i: (0, i)),
        out_shape=jax.ShapeDtypeStruct((tokens, ys * cols), BF16),
        compiler_params=params(),
        cost_estimate=pl.CostEstimate(flops=2 * tokens * depth * ys * cols, bytes_accessed=6 * a.size + 2 * depth * ys * cols, transcendentals=0),
    )(a, w, resid)


def gate_up_kernel(x_ref, gain_ref, wg_ref, wu_ref, *refs, chunk):
    z_ref, h_ref = refs[-2:]

    @pl.when(pl.program_id(0) == 0)
    def _():
        normalise(x_ref, gain_ref, h_ref, 128)

    depth = wg_ref.shape[0] * wg_ref.shape[2]
    wg = wg_ref[...].reshape(depth, wg_ref.shape[3])
    wu = wu_ref[...].reshape(depth, wu_ref.shape[3])
    for r in range(0, h_ref.shape[0], chunk):
        h = h_ref[r:r + chunk, :]
        gate = dot(h, wg)
        up = dot(h, wu)
        z_ref[r:r + chunk, :] = (gate * jax.nn.sigmoid(gate) * up).astype(BF16)


def gate_up(x, gain, w, hidden, parts=1, part=0, onto=None):
    tokens, width = x.shape
    ys, ms = w.shape[:2]
    rows = width // ys
    block = 512
    per = hidden // block
    in_specs = [
        pl.BlockSpec((tokens, width), lambda i: (0, 0)),
        pl.BlockSpec((1, width), lambda i: (0, 0)),
        pl.BlockSpec((ys, 1, rows, block), lambda i: (0, i // per, 0, i % per)),
        pl.BlockSpec((ys, 1, rows, block), lambda i: (0, i // per, 1, i % per)),
    ]
    operands = [x, gain, w, w]
    aliases = {}
    if onto is not None:
        in_specs.append(pl.BlockSpec(memory_space=pl.ANY))
        operands.append(onto)
        aliases = {4: 0}
    return pl.pallas_call(
        functools.partial(gate_up_kernel, chunk=512),
        grid=(ms * per,),
        in_specs=in_specs,
        out_specs=pl.BlockSpec((tokens, block), lambda i: (part, i)),
        out_shape=jax.ShapeDtypeStruct((parts * tokens, ms * hidden), BF16),
        scratch_shapes=[pltpu.VMEM((tokens, width), BF16)],
        input_output_aliases=aliases,
        compiler_params=params(),
        cost_estimate=pl.CostEstimate(flops=4 * tokens * width * ms * hidden, bytes_accessed=2 * x.size + 4 * width * ms * hidden, transcendentals=tokens * ms * hidden),
    )(*operands)


def down_kernel(place_ref, *refs, count, resids, steps, chunk):
    za, zb, ws = refs[:count], refs[count:2 * count], refs[2 * count:3 * count]
    r_refs, o_ref = refs[3 * count:3 * count + resids], refs[-1]
    half = za[0].shape[1]
    w = jnp.concatenate([w[h * half:(h + 1) * half, :] for h in range(2) for w in ws], axis=0)
    for r in range(0, za[0].shape[0], chunk):
        rows = slice(r, r + chunk)
        z = jnp.concatenate([z[rows, :] for z in za + zb], axis=1)
        resid = r_refs[0][rows, :].astype(F32)
        if resids == 2:
            resid = jnp.where(pl.program_id(0) < steps, resid, r_refs[1][rows, :].astype(F32))
        out = (resid + dot(z, w)).astype(BF16)
        if len(o_ref.shape) == 4:
            positions = o_ref.shape[2]
            o_ref[r // positions:(r + chunk) // positions, 0] = out.reshape(chunk // positions, positions, out.shape[1])
        else:
            o_ref[rows, :] = out


def down(place, za, zb, ws, resids, split, other=0, part=0, parts=1, onto=None):
    tokens = za.shape[0]
    width = resids[0].shape[1]
    whole = not isinstance(ws, (list, tuple))
    count = ws.shape[1] if whole else len(ws)
    halves = ws.shape[0] if whole else 1
    cols = ws.shape[3] if whole else ws[0].shape[1]
    half = za.shape[1] // count
    block, rows = 256, 1024
    per = cols // block
    steps = halves * per

    def column(i, place):
        y = i // per % halves if whole else place[1] ^ other
        return (y * parts + part) * per + i % per

    def source(k, place):
        return k if whole else place[0] ^ k

    z_specs = [pl.BlockSpec((rows, half), lambda i, place, k=k: (i // steps, source(k, place))) for k in range(count)]
    in_specs = z_specs + z_specs
    if whole:
        in_specs += [pl.BlockSpec((None, None, 2 * half, block), lambda i, place, k=k: (i // per % halves, k, 0, i % per)) for k in range(count)]
        operands = [za] * count + [zb] * count + [ws] * count + list(resids)
    else:
        in_specs += [pl.BlockSpec((2 * half, block), lambda i, place: (0, i % per))] * count
        operands = [za] * count + [zb] * count + list(ws) + list(resids)
    if len(resids) == 1:
        in_specs += [pl.BlockSpec((rows, block), lambda i, place: (i // steps, column(i, place)))]
    else:
        in_specs += [pl.BlockSpec((rows, block), lambda i, place: (0, column(i, place)))] * len(resids)
    aliases = {}
    if onto is not None:
        in_specs.append(pl.BlockSpec(memory_space=pl.ANY))
        aliases = {1 + len(operands): 0}
        operands.append(onto)
    if split:
        out_spec = pl.BlockSpec((split, 1, rows // split, block), lambda i, place: (0, i // steps, 0, column(i, place)))
        out_shape = (split, tokens // rows, rows // split, width)
    else:
        out_spec = pl.BlockSpec((rows, block), lambda i, place: (i // steps, column(i, place)))
        out_shape = (tokens, width)
    return pl.pallas_call(
        functools.partial(down_kernel, count=count, resids=len(resids), steps=steps, chunk=512),
        grid_spec=pltpu.PrefetchScalarGridSpec(
            num_scalar_prefetch=1,
            grid=(tokens // rows * steps,),
            in_specs=in_specs,
            out_specs=out_spec,
        ),
        out_shape=jax.ShapeDtypeStruct(out_shape, BF16),
        input_output_aliases=aliases,
        compiler_params=params(),
        cost_estimate=pl.CostEstimate(flops=4 * tokens * za.shape[1] * halves * cols, bytes_accessed=4 * za.size + 4 * za.shape[1] * halves * cols, transcendentals=0),
    )(place, *operands)


def down_last_kernel(place_ref, *refs, count, steps):
    za, zb = refs[:count], refs[count:2 * count]
    groups = [refs[(2 + g) * count:(3 + g) * count] for g in range(3)]
    r_refs, o_ref = refs[5 * count:5 * count + 2], refs[-1]
    half = za[0].shape[1]
    step = pl.program_id(0) % steps
    first = pl.program_id(0) < 2 * steps

    def run(ws):
        w = jnp.concatenate([w[h * half:(h + 1) * half, :] for h in range(2) for w in ws], axis=0)
        z = jnp.concatenate([z[...] for z in za + zb], axis=1)
        resid = jnp.where(first, r_refs[0][...].astype(F32), r_refs[1][...].astype(F32))
        out = (resid + dot(z, w)).astype(BF16)
        o_ref[...] = out.reshape(o_ref.shape)

    for g, here in enumerate((step < 2, jnp.logical_and(step >= 2, step < 4), step >= 4)):
        pl.when(here)(functools.partial(run, groups[g]))


def down_last(place, za, zb, own, other, rest, resids, sources):
    tokens = za.shape[0]
    width = resids[0].shape[1]
    count = len(own)
    half = za.shape[1] // count
    block, rows = 256, 512
    steps = width // block
    positions = tokens // 2 // sources
    assert rest.shape[3] == own[0].shape[1] == 2 * block and rest.shape[0] == 2 and rows * 4 == tokens

    def rest_block(j):
        t = jnp.maximum(j - 4, 0)
        return t // 2, t % 2

    def column(i, place):
        j = i % steps
        y, c = rest_block(j)
        side = jnp.where(j < 2, place[1], place[1] ^ 1)
        return jnp.where(j < 4, side * 4 + j % 2, y * 4 + 2 + c)

    def rest_spec(k):
        def index(i, place):
            y, c = rest_block(i % steps)
            return y, place[0] ^ k, 0, c

        return pl.BlockSpec((None, None, 2 * half, block), index)

    in_specs = [pl.BlockSpec((rows, half), lambda i, place, k=k: (i // steps, place[0] ^ k)) for k in range(count)] * 2
    in_specs += [pl.BlockSpec((2 * half, block), lambda i, place: (0, jnp.minimum(i % steps, 1)))] * count
    in_specs += [pl.BlockSpec((2 * half, block), lambda i, place: (0, jnp.clip(i % steps - 2, 0, 1)))] * count
    in_specs += [rest_spec(k) for k in range(count)]
    in_specs += [pl.BlockSpec((rows, block), lambda i, place: (i // steps % 2, column(i, place)))] * 2
    return pl.pallas_call(
        functools.partial(down_last_kernel, count=count, steps=steps),
        grid_spec=pltpu.PrefetchScalarGridSpec(
            num_scalar_prefetch=1,
            grid=(tokens // rows * steps,),
            in_specs=in_specs,
            out_specs=pl.BlockSpec((rows // positions, 1, positions, block), lambda i, place: (i // steps % 2, i // steps // 2, 0, column(i, place))),
        ),
        out_shape=jax.ShapeDtypeStruct((sources, 2, positions, width), BF16),
        compiler_params=params(),
        cost_estimate=pl.CostEstimate(flops=4 * tokens * za.shape[1] * width, bytes_accessed=4 * za.size + 4 * za.shape[1] * width, transcendentals=0),
        name="down_last",
    )(place, *[za] * count, *[zb] * count, *own, *other, *[rest] * count, *resids)


def solution(mesh):
    act_spec = P('fsdp', 'model', None)
    col_spec = P(None, 'fsdp', 'model')
    row_spec = P(None, 'model', 'fsdp')
    ys, ms = mesh.shape['fsdp'], mesh.shape['model']

    def gather(block):
        full = lax.all_gather(block, ('fsdp', 'model'), axis=0, tiled=False)
        return full.reshape((ys, ms) + block.shape)

    def exchange(tokens):
        return lax.all_to_all(tokens, 'model', split_axis=0, concat_axis=0, tiled=True)

    def swap(block, axis, bit):
        return lax.ppermute(block, axis, [(i, i ^ bit) for i in range(mesh.shape[axis])])

    def spread(block):
        across = swap(block, 'model', 2)
        over, over_across = swap(block, 'fsdp', 1), swap(across, 'fsdp', 1)
        partners = [swap(b, 'model', 1) for b in (block, across, over, over_across)]
        return (block, partners[0], across, partners[1]), (over, partners[2], over_across, partners[3])

    def device_step(x_in, gain_attn, gain_mlp, rope_cos, rope_sin, w_q, w_k, w_v, w_o, w_gate, w_up, w_down):
        layers = w_q.shape[0]
        half = w_gate.shape[2] // 2
        place = jnp.stack([lax.axis_index('model'), lax.axis_index('fsdp')]).astype(jnp.int32)
        seqs = x_in.shape[0] // ms
        x = exchange(x_in)
        gathered = []
        for l in range(layers):
            last = l == layers - 1
            block = jnp.concatenate([w_q[l], w_k[l], w_v[l]], axis=1)
            wqkv = gather(block)
            if last:
                wo = gather(w_o[l])
            block = jnp.concatenate([w_gate[l, :, :half], w_up[l, :, :half]] + ([] if last else [w_o[l]]), axis=0)
            wgua = gather(block)
            if not last:
                wo = wgua
            block = jnp.concatenate([w_gate[l, :, half:], w_up[l, :, half:]], axis=0)
            wgub = gather(block)
            cols = w_down.shape[2] // (2 if last else 1)
            block = w_down[l, :, :cols]
            rest = w_down[l, :, cols:]
            wd = spread(block)
            gathered.append((wqkv, wo, wgua, wgub, wd, gather(rest) if last else None))

        x = x.reshape(-1, x.shape[2])
        cos = jnp.tile(rope_cos, (1, 4))
        sin = jnp.tile(jnp.concatenate([-rope_sin, rope_sin], axis=1), (1, 2))
        for l in range(layers):
            wqkv, wo, wgua, wgub, (own, other), rest = gathered[l]
            gain = gain_mlp[l][None]
            wo_block = wo.shape[2] // w_o.shape[1] - 1
            q, k, v = project_qkv(x, gain_attn[l][None], cos, sin, wqkv)
            x4 = x.reshape(ms, seqs, -1, x.shape[1])
            if l < layers - 1:
                o = attend(q, k, v, ms, seqs, None)
                resids = [out_proj(o, wo, wo_block, x4, None)]
                split = None
            else:
                resids, split = [], ms
                for i in range(seqs):
                    o = attend(q, k, v, ms, seqs, i)
                    m = out_proj(o, wo, wo_block, x4, i)
                    resids.append(exchange(m.reshape(ms, -1, m.shape[1])).reshape(m.shape))
            za = zb = None
            for i, m in enumerate(resids):
                za = gate_up(m, gain, wgua, half, len(resids), i, za)
            for i, m in enumerate(resids):
                zb = gate_up(m, gain, wgub, half, len(resids), i, zb)
            if rest is None:
                x = down(place, za, zb, own, resids, split)
                x = down(place, za, zb, other, resids, split, 1, onto=x)
            else:
                x = down_last(place, za, zb, own, other, rest, resids, ms)
        return x.reshape(x_in.shape)

    return jax.shard_map(device_step, mesh=mesh, in_specs=(act_spec, P(), P(), P(), P(), col_spec, col_spec, col_spec, row_spec, col_spec, col_spec, row_spec), out_specs=act_spec, check_vma=False)
```

```python
import functools
import math

import jax
import jax.numpy as jnp
from jax import lax
from jax.experimental import pallas as pl
from jax.experimental.pallas import tpu as pltpu
from jax.sharding import PartitionSpec as P


EPS = 1e-5
VMEM = 60 * 1024 * 1024
F32 = jnp.float32
BF16 = jnp.bfloat16


def dot(a, b):
    return jnp.dot(a, b, preferred_element_type=F32)


def params():
    return pltpu.CompilerParams(dimension_semantics=("arbitrary",), vmem_limit_bytes=VMEM)


def normalise(x_ref, gain_ref, h_ref, chunk):
    def step(i, carry):
        rows = pl.ds(pl.multiple_of(i * chunk, chunk), chunk)
        x = x_ref[rows, :].astype(F32)
        mean_sq = jnp.mean(x * x, axis=-1, keepdims=True)
        h_ref[rows, :] = (x * lax.rsqrt(mean_sq + EPS) * gain_ref[...]).astype(BF16)
        return carry

    lax.fori_loop(0, x_ref.shape[0] // chunk, step, 0)


def rotate(x, cos, sin):
    lane = lax.broadcasted_iota(jnp.int32, x.shape, 1)
    swapped = jnp.where(lane % 64 < 32, pltpu.roll(x, 96, 1), pltpu.roll(x, 32, 1))
    return x * cos + swapped * sin


def qkv_kernel(x_ref, gain_ref, cos_ref, sin_ref, w_ref, q_ref, k_ref, v_ref, h_ref):
    @pl.when(pl.program_id(0) == 0)
    def _():
        normalise(x_ref, gain_ref, h_ref, 128)

    w = w_ref[...].reshape(w_ref.shape[0] * w_ref.shape[2], w_ref.shape[3])
    q_width, k_width = q_ref.shape[1], k_ref.shape[1]
    positions = 256
    step = 2 * positions
    for r in range(0, h_ref.shape[0], step):
        rows = slice(r, r + step)
        out = dot(h_ref[rows, :], w).astype(BF16)
        table = slice(r // 2, r // 2 + positions)
        cos, sin = cos_ref[table, :], sin_ref[table, :]
        cos, sin = jnp.concatenate([cos, cos], axis=0), jnp.concatenate([sin, sin], axis=0)
        for c in range(0, q_width, 128):
            q_ref[rows, c:c + 128] = rotate(out[:, c:c + 128].astype(F32), cos, sin).astype(BF16)
        for c in range(0, k_width, 128):
            k_ref[rows, c:c + 128] = rotate(out[:, q_width + c:q_width + c + 128].astype(F32), cos, sin).astype(BF16)
        v_ref[rows, :] = out[:, q_width + k_width:]


def project_qkv(x, gain, cos, sin, w):
    tokens, width = x.shape
    q_width, k_width = 512, 128
    blocks = w.shape[1]
    flops = 2 * tokens * width * blocks * w.shape[3]
    return pl.pallas_call(
        qkv_kernel,
        grid=(blocks,),
        in_specs=[
            pl.BlockSpec((tokens, width), lambda m: (0, 0)),
            pl.BlockSpec((1, width), lambda m: (0, 0)),
            pl.BlockSpec(cos.shape, lambda m: (0, 0)),
            pl.BlockSpec(sin.shape, lambda m: (0, 0)),
            pl.BlockSpec((w.shape[0], 1, w.shape[2], w.shape[3]), lambda m: (0, m, 0, 0)),
        ],
        out_specs=[
            pl.BlockSpec((tokens, q_width), lambda m: (0, m)),
            pl.BlockSpec((tokens, k_width), lambda m: (0, m)),
            pl.BlockSpec((tokens, k_width), lambda m: (0, m)),
        ],
        out_shape=[
            jax.ShapeDtypeStruct((tokens, blocks * q_width), BF16),
            jax.ShapeDtypeStruct((tokens, blocks * k_width), BF16),
            jax.ShapeDtypeStruct((tokens, blocks * k_width), BF16),
        ],
        scratch_shapes=[pltpu.VMEM((tokens, width), BF16)],
        compiler_params=params(),
        cost_estimate=pl.CostEstimate(flops=flops, bytes_accessed=4 * tokens * width + 2 * w.size, transcendentals=0),
        name="qkv",
    )(x, gain, cos, sin, w)


def attention_kernel(q_ref, k_ref, v_ref, o_ref, ks, vs):
    chunks, _, chunk, _ = q_ref.shape
    lo = lax.broadcasted_iota(jnp.int32, (chunk, 128), 1) < 64
    for c in range(chunks):
        rows = slice(c * chunk, (c + 1) * chunk)
        keys = k_ref[c, 0].astype(F32).T.astype(BF16)
        values = v_ref[c, 0].astype(F32)
        swapped = pltpu.roll(values, 64, 1)
        for g in range(2):
            key = keys[64 * g:64 * g + 64, :]
            ks[g, :, rows] = jnp.concatenate([key, key], axis=0)
            first, second = (swapped, values) if g else (values, swapped)
            vs[g, 0, rows, :] = jnp.where(lo, first, 0.0).astype(BF16)
            vs[g, 1, rows, :] = jnp.where(lo, 0.0, second).astype(BF16)
    scale = 64 ** -0.5 * math.log2(math.e)
    row = lax.broadcasted_iota(jnp.int32, (4 * chunk, chunk), 0) % chunk
    col = lax.broadcasted_iota(jnp.int32, (4 * chunk, chunk), 1)
    causal = row >= col

    def group(g, carry):
        for b in range(chunks):
            n = (b + 1) * chunk
            heads = []
            for p in range(2):
                pair = q_ref[b, 0, :, pl.ds(pl.multiple_of(g * 256 + p * 128, 128), 128)].astype(F32)
                heads += [jnp.where(lo, pair, 0.0).astype(BF16), jnp.where(lo, 0.0, pair).astype(BF16)]
            q = jnp.concatenate(heads, axis=0)
            parts = [dot(q, ks[g, :, c * chunk:(c + 1) * chunk]) for c in range(b + 1)]
            parts[b] = jnp.where(causal, parts[b], -jnp.inf)
            top = jnp.max(functools.reduce(jnp.maximum, parts), axis=1, keepdims=True)
            parts = [jnp.exp2((part - top) * scale) for part in parts]
            inverse = 1.0 / jnp.sum(functools.reduce(jnp.add, parts), axis=1, keepdims=True)
            probs = [(part * inverse).astype(BF16) for part in parts]
            values = jnp.concatenate([vs[g, 0, :n, :], vs[g, 1, :n, :]], axis=0)
            for p in range(2):
                even, odd = 2 * p * chunk, (2 * p + 1) * chunk
                pair = jnp.concatenate([x[even:even + chunk] for x in probs] + [x[odd:odd + chunk] for x in probs], axis=1)
                o_ref[b, 0, :, pl.ds(pl.multiple_of(g * 256 + p * 128, 128), 128)] = dot(pair, values).astype(BF16)
        return carry

    lax.fori_loop(0, 2, group, 0)


def attend(q, k, v, chunks, seqs, only):
    tokens = q.shape[0]
    chunk = tokens // (chunks * seqs)
    q4, k4, v4 = (a.reshape(chunks, seqs, chunk, a.shape[1]) for a in (q, k, v))
    seq = chunks * chunk
    blocks = k.shape[1] // 128
    q_width = q.shape[1] // blocks
    heads = q.shape[1] // 64
    count = seqs if only is None else 1
    first = only or 0
    out = pl.pallas_call(
        attention_kernel,
        grid=(count * blocks,),
        in_specs=[
            pl.BlockSpec((chunks, 1, chunk, width), lambda i: (0, first + i // blocks, 0, i % blocks))
            for width in (q_width, 128, 128)
        ],
        out_specs=pl.BlockSpec((chunks, 1, chunk, q_width), lambda i: (0, i // blocks, 0, i % blocks)),
        out_shape=jax.ShapeDtypeStruct((chunks, count, chunk, q.shape[1]), BF16),
        scratch_shapes=[
            pltpu.VMEM((2, 128, seq), BF16),
            pltpu.VMEM((2, 2, seq, 128), BF16),
        ],
        compiler_params=params(),
        cost_estimate=pl.CostEstimate(flops=8 * count * heads * seq * seq * 64, bytes_accessed=5 * count * seq * q.shape[1], transcendentals=count * heads * seq * seq),
    )(q4, k4, v4)
    return out.reshape(count * seq, q.shape[1])


def out_proj_kernel(a_ref, w_ref, r_ref, o_ref, *, chunk):
    w = w_ref[0].reshape(a_ref.shape[1], w_ref.shape[3])
    resid = r_ref[...].reshape(o_ref.shape)
    for r in range(0, a_ref.shape[0], chunk):
        acc = dot(a_ref[r:r + chunk, :], w)
        o_ref[r:r + chunk, :] = (resid[r:r + chunk, :].astype(F32) + acc).astype(BF16)


def out_proj(a, w, row_block, resid, only):
    tokens, depth = a.shape
    ys, ms, _, cols = w.shape
    block = 512
    per = cols // block
    chunks, seqs, chunk, _ = resid.shape
    count = seqs if only is None else 1
    first = only or 0
    return pl.pallas_call(
        functools.partial(out_proj_kernel, chunk=512),
        grid=(ys * per,),
        in_specs=[
            pl.BlockSpec((tokens, depth), lambda i: (0, 0)),
            pl.BlockSpec((1, ms, depth // ms, block), lambda i: (i // per, 0, row_block, i % per)),
            pl.BlockSpec((chunks, count, chunk, block), lambda i: (0, first, 0, i)),
        ],
        out_specs=pl.BlockSpec((tokens, block), lambda i: (0, i)),
        out_shape=jax.ShapeDtypeStruct((tokens, ys * cols), BF16),
        compiler_params=params(),
        cost_estimate=pl.CostEstimate(flops=2 * tokens * depth * ys * cols, bytes_accessed=6 * a.size + 2 * depth * ys * cols, transcendentals=0),
    )(a, w, resid)


def gate_up_kernel(x_ref, gain_ref, wg_ref, wu_ref, *refs, chunk):
    z_ref, h_ref = refs[-2:]

    @pl.when(pl.program_id(0) == 0)
    def _():
        normalise(x_ref, gain_ref, h_ref, 128)

    depth = wg_ref.shape[2]

    def project(rows, w_ref):
        return functools.reduce(jnp.add, [dot(h_ref[rows, y * depth:(y + 1) * depth], w_ref[y, 0]) for y in range(w_ref.shape[0])])

    for r in range(0, h_ref.shape[0], chunk):
        gate = project(slice(r, r + chunk), wg_ref)
        up = project(slice(r, r + chunk), wu_ref)
        z_ref[r:r + chunk, :] = (gate * jax.nn.sigmoid(gate) * up).astype(BF16)


def gate_up(x, gain, w, hidden, parts=1, part=0, onto=None):
    tokens, width = x.shape
    ys, ms = w.shape[:2]
    rows = width // ys
    block = 512
    per = hidden // block
    in_specs = [
        pl.BlockSpec((tokens, width), lambda i: (0, 0)),
        pl.BlockSpec((1, width), lambda i: (0, 0)),
        pl.BlockSpec((ys, 1, rows, block), lambda i: (0, i // per, 0, i % per)),
        pl.BlockSpec((ys, 1, rows, block), lambda i: (0, i // per, 1, i % per)),
    ]
    operands = [x, gain, w, w]
    aliases = {}
    if onto is not None:
        in_specs.append(pl.BlockSpec(memory_space=pl.ANY))
        operands.append(onto)
        aliases = {4: 0}
    return pl.pallas_call(
        functools.partial(gate_up_kernel, chunk=512),
        grid=(ms * per,),
        in_specs=in_specs,
        out_specs=pl.BlockSpec((tokens, block), lambda i: (part, i)),
        out_shape=jax.ShapeDtypeStruct((parts * tokens, ms * hidden), BF16),
        scratch_shapes=[pltpu.VMEM((tokens, width), BF16)],
        input_output_aliases=aliases,
        compiler_params=params(),
        cost_estimate=pl.CostEstimate(flops=4 * tokens * width * ms * hidden, bytes_accessed=2 * x.size + 4 * width * ms * hidden, transcendentals=tokens * ms * hidden),
    )(*operands)


def down_dot(za, zb, ws, rows):
    half = za[0].shape[1]
    terms = [dot(z[rows, :], w[h * half:(h + 1) * half, :]) for h, zs in enumerate((za, zb)) for z, w in zip(zs, ws)]
    return functools.reduce(jnp.add, terms)


def down_kernel(place_ref, *refs, count, resids, steps, chunk):
    za, zb, ws = refs[:count], refs[count:2 * count], refs[2 * count:3 * count]
    r_refs, o_ref = refs[3 * count:3 * count + resids], refs[-1]
    for r in range(0, za[0].shape[0], chunk):
        rows = slice(r, r + chunk)
        resid = r_refs[0][rows, :].astype(F32)
        if resids == 2:
            resid = jnp.where(pl.program_id(0) < steps, resid, r_refs[1][rows, :].astype(F32))
        out = (resid + down_dot(za, zb, ws, rows)).astype(BF16)
        if len(o_ref.shape) == 4:
            positions = o_ref.shape[2]
            o_ref[r // positions:(r + chunk) // positions, 0] = out.reshape(chunk // positions, positions, out.shape[1])
        else:
            o_ref[rows, :] = out


def down(place, za, zb, ws, resids, split, other=0, part=0, parts=1, onto=None):
    tokens = za.shape[0]
    width = resids[0].shape[1]
    whole = not isinstance(ws, (list, tuple))
    count = ws.shape[1] if whole else len(ws)
    halves = ws.shape[0] if whole else 1
    cols = ws.shape[3] if whole else ws[0].shape[1]
    half = za.shape[1] // count
    block, rows = 256, 1024
    per = cols // block
    steps = halves * per

    def column(i, place):
        y = i // per % halves if whole else place[1] ^ other
        return (y * parts + part) * per + i % per

    def source(k, place):
        return k if whole else place[0] ^ k

    z_specs = [pl.BlockSpec((rows, half), lambda i, place, k=k: (i // steps, source(k, place))) for k in range(count)]
    in_specs = z_specs + z_specs
    if whole:
        in_specs += [pl.BlockSpec((None, None, 2 * half, block), lambda i, place, k=k: (i // per % halves, k, 0, i % per)) for k in range(count)]
        operands = [za] * count + [zb] * count + [ws] * count + list(resids)
    else:
        in_specs += [pl.BlockSpec((2 * half, block), lambda i, place: (0, i % per))] * count
        operands = [za] * count + [zb] * count + list(ws) + list(resids)
    if len(resids) == 1:
        in_specs += [pl.BlockSpec((rows, block), lambda i, place: (i // steps, column(i, place)))]
    else:
        in_specs += [pl.BlockSpec((rows, block), lambda i, place: (0, column(i, place)))] * len(resids)
    aliases = {}
    if onto is not None:
        in_specs.append(pl.BlockSpec(memory_space=pl.ANY))
        aliases = {1 + len(operands): 0}
        operands.append(onto)
    if split:
        out_spec = pl.BlockSpec((split, 1, rows // split, block), lambda i, place: (0, i // steps, 0, column(i, place)))
        out_shape = (split, tokens // rows, rows // split, width)
    else:
        out_spec = pl.BlockSpec((rows, block), lambda i, place: (i // steps, column(i, place)))
        out_shape = (tokens, width)
    return pl.pallas_call(
        functools.partial(down_kernel, count=count, resids=len(resids), steps=steps, chunk=512),
        grid_spec=pltpu.PrefetchScalarGridSpec(
            num_scalar_prefetch=1,
            grid=(tokens // rows * steps,),
            in_specs=in_specs,
            out_specs=out_spec,
        ),
        out_shape=jax.ShapeDtypeStruct(out_shape, BF16),
        input_output_aliases=aliases,
        compiler_params=params(),
        cost_estimate=pl.CostEstimate(flops=4 * tokens * za.shape[1] * halves * cols, bytes_accessed=4 * za.size + 4 * za.shape[1] * halves * cols, transcendentals=0),
    )(place, *operands)


def down_last_kernel(place_ref, *refs, count, steps):
    za, zb = refs[:count], refs[count:2 * count]
    groups = [refs[(2 + g) * count:(3 + g) * count] for g in range(3)]
    r_refs, o_ref = refs[5 * count:5 * count + 2], refs[-1]
    step = pl.program_id(0) % steps
    first = pl.program_id(0) < 2 * steps

    def run(ws):
        resid = jnp.where(first, r_refs[0][...].astype(F32), r_refs[1][...].astype(F32))
        out = (resid + down_dot(za, zb, ws, slice(None))).astype(BF16)
        o_ref[...] = out.reshape(o_ref.shape)

    for g, here in enumerate((step < 2, jnp.logical_and(step >= 2, step < 4), step >= 4)):
        pl.when(here)(functools.partial(run, groups[g]))


def down_last(place, za, zb, own, other, rest, resids, sources):
    tokens = za.shape[0]
    width = resids[0].shape[1]
    count = len(own)
    half = za.shape[1] // count
    block, rows = 256, 512
    steps = width // block
    positions = tokens // 2 // sources
    assert rest.shape[3] == own[0].shape[1] == 2 * block and rest.shape[0] == 2 and rows * 4 == tokens

    def rest_block(j):
        t = jnp.maximum(j - 4, 0)
        return t // 2, t % 2

    def column(i, place):
        j = i % steps
        y, c = rest_block(j)
        side = jnp.where(j < 2, place[1], place[1] ^ 1)
        return jnp.where(j < 4, side * 4 + j % 2, y * 4 + 2 + c)

    def rest_spec(k):
        def index(i, place):
            y, c = rest_block(i % steps)
            return y, place[0] ^ k, 0, c

        return pl.BlockSpec((None, None, 2 * half, block), index)

    in_specs = [pl.BlockSpec((rows, half), lambda i, place, k=k: (i // steps, place[0] ^ k)) for k in range(count)] * 2
    in_specs += [pl.BlockSpec((2 * half, block), lambda i, place: (0, jnp.minimum(i % steps, 1)))] * count
    in_specs += [pl.BlockSpec((2 * half, block), lambda i, place: (0, jnp.clip(i % steps - 2, 0, 1)))] * count
    in_specs += [rest_spec(k) for k in range(count)]
    in_specs += [pl.BlockSpec((rows, block), lambda i, place: (i // steps % 2, column(i, place)))] * 2
    return pl.pallas_call(
        functools.partial(down_last_kernel, count=count, steps=steps),
        grid_spec=pltpu.PrefetchScalarGridSpec(
            num_scalar_prefetch=1,
            grid=(tokens // rows * steps,),
            in_specs=in_specs,
            out_specs=pl.BlockSpec((rows // positions, 1, positions, block), lambda i, place: (i // steps % 2, i // steps // 2, 0, column(i, place))),
        ),
        out_shape=jax.ShapeDtypeStruct((sources, 2, positions, width), BF16),
        compiler_params=params(),
        cost_estimate=pl.CostEstimate(flops=4 * tokens * za.shape[1] * width, bytes_accessed=4 * za.size + 4 * za.shape[1] * width, transcendentals=0),
        name="down_last",
    )(place, *[za] * count, *[zb] * count, *own, *other, *[rest] * count, *resids)


def solution(mesh):
    act_spec = P('fsdp', 'model', None)
    col_spec = P(None, 'fsdp', 'model')
    row_spec = P(None, 'model', 'fsdp')
    ys, ms = mesh.shape['fsdp'], mesh.shape['model']

    def gather(block):
        full = lax.all_gather(block, ('fsdp', 'model'), axis=0, tiled=False)
        return full.reshape((ys, ms) + block.shape)

    def exchange(tokens):
        return lax.all_to_all(tokens, 'model', split_axis=0, concat_axis=0, tiled=True)

    def swap(block, axis, bit):
        return lax.ppermute(block, axis, [(i, i ^ bit) for i in range(mesh.shape[axis])])

    def spread(block):
        across = swap(block, 'model', 2)
        over, over_across = swap(block, 'fsdp', 1), swap(across, 'fsdp', 1)
        partners = [swap(b, 'model', 1) for b in (block, across, over, over_across)]
        return (block, partners[0], across, partners[1]), (over, partners[2], over_across, partners[3])

    def device_step(x_in, gain_attn, gain_mlp, rope_cos, rope_sin, w_q, w_k, w_v, w_o, w_gate, w_up, w_down):
        layers = w_q.shape[0]
        half = w_gate.shape[2] // 2
        place = jnp.stack([lax.axis_index('model'), lax.axis_index('fsdp')]).astype(jnp.int32)
        seqs = x_in.shape[0] // ms
        x = exchange(x_in)
        gathered = []
        for l in range(layers):
            last = l == layers - 1
            block = jnp.concatenate([w_q[l], w_k[l], w_v[l]], axis=1)
            wqkv = gather(block)
            if last:
                wo = gather(w_o[l])
            block = jnp.concatenate([w_gate[l, :, :half], w_up[l, :, :half]] + ([] if last else [w_o[l]]), axis=0)
            wgua = gather(block)
            if not last:
                wo = wgua
            block = jnp.concatenate([w_gate[l, :, half:], w_up[l, :, half:]], axis=0)
            wgub = gather(block)
            cols = w_down.shape[2] // (2 if last else 1)
            block = w_down[l, :, :cols]
            rest = w_down[l, :, cols:]
            wd = spread(block)
            gathered.append((wqkv, wo, wgua, wgub, wd, gather(rest) if last else None))

        x = x.reshape(-1, x.shape[2])
        cos = jnp.tile(rope_cos, (1, 4))
        sin = jnp.tile(jnp.concatenate([-rope_sin, rope_sin], axis=1), (1, 2))
        for l in range(layers):
            wqkv, wo, wgua, wgub, (own, other), rest = gathered[l]
            gain = gain_mlp[l][None]
            wo_block = wo.shape[2] // w_o.shape[1] - 1
            q, k, v = project_qkv(x, gain_attn[l][None], cos, sin, wqkv)
            x4 = x.reshape(ms, seqs, -1, x.shape[1])
            if l < layers - 1:
                o = attend(q, k, v, ms, seqs, None)
                resids = [out_proj(o, wo, wo_block, x4, None)]
                split = None
            else:
                resids, split = [], ms
                for i in range(seqs):
                    o = attend(q, k, v, ms, seqs, i)
                    m = out_proj(o, wo, wo_block, x4, i)
                    resids.append(exchange(m.reshape(ms, -1, m.shape[1])).reshape(m.shape))
            za = zb = None
            for i, m in enumerate(resids):
                za = gate_up(m, gain, wgua, half, len(resids), i, za)
            for i, m in enumerate(resids):
                zb = gate_up(m, gain, wgub, half, len(resids), i, zb)
            if rest is None:
                x = down(place, za, zb, own, resids, split)
                x = down(place, za, zb, other, resids, split, 1, onto=x)
            else:
                x = down_last(place, za, zb, own, other, rest, resids, ms)
        return x.reshape(x_in.shape)

    return jax.shard_map(device_step, mesh=mesh, in_specs=(act_spec, P(), P(), P(), P(), col_spec, col_spec, col_spec, row_spec, col_spec, col_spec, row_spec), out_specs=act_spec, check_vma=False)
```
